32 devices in a mesh: fsdp: 8 (over y, x, core), seq: 4 (over z).
Axes of the slice: x: 2, y: 2, z: 4, core: 2. Of those that a mesh axis runs over, the one named last changes fastest.
Arguments:
- tokens: bfloat16 [8, 2048, 4096], P('fsdp', 'seq'), may hold values from -72 to 72
- norm_gain: float32 [4096], replicated, may hold values from 0.1 to 1.9
- lru_proj: bfloat16 [4096, 2048], P(('fsdp', 'seq')), may hold values from -0.09375 to 0.09375
- gelu_proj: bfloat16 [4096, 2048], P(('fsdp', 'seq')), may hold values from -0.09375 to 0.09375
- conv_weight: float32 [4, 2048], replicated, may hold values from -3 to 3
- conv_bias: float32 [2048], replicated, may hold values from -3 to 3
- gate_weights: bfloat16 [2048, 512], P('seq'), may hold values from -0.375 to 0.375
- gate_bias: float32 [2, 2048], replicated, may hold values from -4 to 4
- decay_param: float32 [2048], replicated, may hold values from -13 to -2
Outputs:
- recurrent_out: bfloat16 [8, 2048, 2048], P('fsdp', 'seq')
The draws below stay inside these ranges and needn't reach their ends.
All inputs are finite; a program needn't handle non-finite values.
Results may differ from the reference program's by a relative error of at most 0.0051.
Values may be sent and summed in bfloat16 or wider, within the bound.
A program may use at most 128 MiB of HBM per device.

```python
import math
import jax
import jax.numpy as jnp
from jax import lax

D = 4096
BW = 256
H = 8
CONV = 4
TOK_DEV = 512
C = 2048
LENGTH = 2048
SEQS = 8


def draw_tokens(key, part):
    keys = jax.random.split(key, 3)
    shape = (SEQS, LENGTH, D)
    column_scale = jnp.exp(jax.random.uniform(keys[0], (D,), jnp.float32, math.log(0.3), math.log(3.0)))
    row_scale = jnp.exp(jax.random.uniform(keys[1], (SEQS, LENGTH, 1), jnp.float32, math.log(0.3), math.log(3.0)))
    base = jnp.clip(jax.random.normal(keys[2], shape, jnp.float32), -3.0, 3.0)
    return (base * row_scale * column_scale).astype(jnp.bfloat16)


def draw_decay_param(key, part):
    keys = jax.random.split(key, 3)
    shortest = min(40, TOK_DEV)
    slow_rate = jnp.exp(jax.random.uniform(keys[0], (C,), jnp.float32, math.log(0.05 / LENGTH), math.log(0.5 / LENGTH)))
    fast_rate = jnp.exp(jax.random.uniform(keys[1], (C,), jnp.float32, math.log(0.2 / shortest), math.log(0.5 / shortest)))
    share = 0.5
    picked = jax.random.uniform(keys[2], (C,), jnp.float32) < share
    rate = jnp.where(picked, fast_rate, slow_rate)
    return jnp.log(jnp.expm1(rate)).astype(jnp.float32)


def block_levels(key, dims, cuts, smallest, high):
    def one(position, blocks):
        draws = jax.random.uniform(jax.random.fold_in(jax.random.fold_in(key, 6), position), (blocks,), jnp.float32, smallest / len(cuts), high / len(cuts))
        return jnp.repeat(jnp.exp(draws), dims[position] // blocks).reshape((-1,) + (1,) * (len(dims) - position - 1))

    factor_of = one(*cuts[0])
    for cut in cuts[1:]:
        factor_of = factor_of * one(*cut)
    return factor_of


def noise(stream_key, extent, width, bound, cuts=(), kind=jnp.bfloat16):
    values = jax.random.normal(stream_key, extent, jnp.float32) * width
    if len(cuts) > 0:
        values = block_levels(stream_key, extent, cuts, -0.22, 0.18) * values
    return jnp.clip(values, min=-bound, max=bound).astype(kind)


def setup_inputs(seed: int = 0) -> dict:
    streams_of = jax.random.split(jax.random.key(seed), 10)
    return {
        "tokens": draw_tokens(jax.random.fold_in(streams_of[9], 71), 0),
        "norm_gain": jnp.clip(1.0 + 0.18 * jax.random.normal(streams_of[1], (D,), jnp.float32), 0.1, 1.9),
        "lru_proj": noise(streams_of[2], (D, C), D ** -0.5, 0.09375, ((0, 32),)),
        "gelu_proj": noise(streams_of[3], (D, C), D ** -0.5, 0.09375, ((0, 32),)),
        "conv_weight": noise(streams_of[4], (CONV, C), 0.5, 3.0, (), jnp.float32),
        "conv_bias": noise(streams_of[5], (C,), 0.5, 3.0, (), jnp.float32),
        "gate_weights": noise(streams_of[6], (C, 2 * BW), BW ** -0.5, 0.375, ((0, 4),)),
        "gate_bias": noise(streams_of[7], (2, C), 1.0, 4.0, (), jnp.float32),
        "decay_param": draw_decay_param(jax.random.fold_in(streams_of[9], 71), 0),
    }


def reference(tokens, norm_gain, lru_proj, gelu_proj, conv_weight, conv_bias, gate_weights, gate_bias, decay_param):

    def one_sequence(rows):
        values = rows.astype(jnp.float32)
        mean_square = lax.optimization_barrier(jnp.mean(values * values, axis=-1, keepdims=True))
        normed = (values * lax.rsqrt(mean_square + 1e-06) * norm_gain).astype(jnp.bfloat16)
        recurrent_in = jnp.dot(normed, lru_proj, preferred_element_type=jnp.float32).astype(jnp.bfloat16)
        gelu_in = jnp.dot(normed, gelu_proj, preferred_element_type=jnp.float32)
        padded = jnp.concatenate([jnp.zeros((CONV - 1, C), jnp.bfloat16), recurrent_in], axis=0)
        conv_sum = jnp.zeros((LENGTH, C), jnp.float32) + conv_bias
        for tap_index in range(CONV):
            begin = CONV - 1 - tap_index
            conv_sum = conv_sum + conv_weight[tap_index] * padded[begin:begin + LENGTH].astype(jnp.float32)
        conv_out = conv_sum.astype(jnp.bfloat16)
        gate_all = jnp.einsum('lhi,hij->lhj', conv_out.astype(jnp.float32).reshape(LENGTH, H, BW), gate_weights.astype(jnp.float32).reshape(H, BW, 2 * BW))
        input_gate = jax.nn.sigmoid(gate_all[:, :, :BW].reshape(LENGTH, C) + gate_bias[0])
        recur_gate = jax.nn.sigmoid(gate_all[:, :, BW:].reshape(LENGTH, C) + gate_bias[1])
        log_decay = -8.0 * jax.nn.softplus(decay_param) * recur_gate
        decay = jnp.exp(log_decay)
        driven = jnp.sqrt(-jnp.expm1(2.0 * log_decay)) * input_gate * conv_out.astype(jnp.float32)

        def advance(state, inputs):
            decay_now, driven_now = inputs
            state = decay_now * state + driven_now
            return (state, state)
        unused, states = lax.scan(advance, jnp.zeros((C,), jnp.float32), (decay, driven))
        return (states * jax.nn.gelu(gelu_in, approximate=True)).astype(jnp.bfloat16)
    return lax.map(one_sequence, tokens)
```

```python
import functools

import jax
import jax.numpy as jnp
from jax import lax
from jax.experimental import pallas as pl
from jax.experimental.pallas import tpu as pltpu
from jax.sharding import PartitionSpec as P

MESH = pl.DeviceIdType.MESH
LANES = 128
VMEM_BYTES = 66_000_000


def normalise(normed_ref, gain_ref, part, parts):
    rows = 32

    def body(i, _):
        at = pl.ds(pl.multiple_of(i * rows, rows), rows)
        values = normed_ref[at, :].astype(jnp.float32)
        mean_square = jnp.mean(values * values, axis=-1, keepdims=True)
        normed_ref[at, :] = (values * lax.rsqrt(mean_square + 1e-06) * gain_ref[...]).astype(jnp.bfloat16)
        return 0

    blocks = normed_ref.shape[0] // rows // parts
    lax.fori_loop(part * blocks, (part + 1) * blocks, body, 0)


LEAD = 4
GAP = 2
NORM_PARTS = 8


def branch_kernel(
    nz,
    tokens_ref, gain_ref, lru_ref, gelu_ref, gate_ref,
    weight_ref, bias_ref, gate_bias_ref, decay_ref,
    out_ref,
    w_ref, normed_ref, rec_ref, table_ref, before_ref, padded_ref, a_ref, b_ref,
    end_ref, carry_ref, start_ref,
    own_sem, send_sem, core_send, gate_send, gate_core_send, tail_send, carry_send,
    z_recv, d_recv, gate_recv, gate_core_recv, x_own, y_own, x_rest, y_rest,
    near_x, near_y, far_x, far_y, core_recv, tail_recv, carry_recv,
):
    f = lax.axis_index("fsdp")
    z = lax.axis_index("seq")
    c, x, y = f % 2, (f // 2) % 2, f // 4
    fx, fy, fc = f + 2 - 4 * x, f + 4 - 8 * y, f + 1 - 2 * c
    fd = fx + 4 - 8 * y
    shard = lru_ref.shape[0]
    line = shard * nz
    half = shard // 2
    chunks = w_ref.shape[0]
    split = chunks // 2
    gate_rows = gate_ref.shape[0]
    gate_steps = split // 2
    piece = gate_rows // 2 // gate_steps
    rows = normed_ref.shape[0]
    channels = table_ref.shape[1] // 2
    heads = rec_ref.shape[1] // channels
    pieces = channels // LANES
    taps = weight_ref.shape[0]
    lead = before_ref.shape[0]
    last = nz - 1
    reach = nz - 2
    at_end = (z == 0) | (z == last)

    def remote(src, send, recv, device):
        return pltpu.make_async_remote_copy(
            src_ref=src, dst_ref=src, send_sem=send, recv_sem=recv,
            device_id=device, device_id_type=MESH,
        )

    own = pl.ds(pl.multiple_of((f * nz + z) * shard, shard), shard)
    for t in range(chunks):
        src = lru_ref if t < split else gelu_ref
        cols = pl.ds((t % split) * LANES, LANES)
        pltpu.make_async_copy(src.at[:, cols], w_ref.at[t, own], own_sem.at[0]).start()
    own_gate = pl.ds(pl.multiple_of(z * gate_rows, gate_rows), gate_rows)
    gate_copy = pltpu.make_async_copy(gate_ref, table_ref.at[own_gate], own_sem.at[1])
    gate_copy.start()
    token_copy = pltpu.make_async_copy(tokens_ref, normed_ref, own_sem.at[2])
    token_copy.start()

    barrier = pltpu.get_barrier_semaphore()
    for device in ((fx, z), (fy, z), (fc, z)):
        pl.semaphore_signal(barrier, inc=1, device_id=device, device_id_type=MESH)

    @pl.when(z > 0)
    def _():
        pl.semaphore_signal(barrier, inc=1, device_id=(f, z - 1), device_id_type=MESH)

    @pl.when(z < last)
    def _():
        pl.semaphore_signal(barrier, inc=1, device_id=(f, z + 1), device_id_type=MESH)

    for k in range(nz):
        @pl.when(z == k)
        def _():
            pl.semaphore_wait(barrier, 3 + int(k > 0) + int(k < last))

    pltpu.make_async_copy(w_ref.at[:, own], w_ref.at[:, own], own_sem.at[0]).wait()
    gate_copy.wait()

    def unit(t, owner, k, first=0, size=shard):
        start = (owner * nz + k) * shard + first
        return w_ref.at[t, pl.ds(pl.multiple_of(start, half), size)]

    def whole_line(t, owner):
        return w_ref.at[t, pl.ds(pl.multiple_of(owner * line, line), line)]

    def gate_of(t, source):
        first = source * gate_rows + c * (gate_rows // 2) + t * piece
        return table_ref.at[pl.ds(pl.multiple_of(first, piece), piece)]

    def along_z(t, k, target):
        remote(unit(t, f, k), send_sem.at[t], z_recv.at[t, k], (f, target)).start()

        @pl.when(t < gate_steps)
        def _():
            remote(gate_of(t, k), gate_send.at[t], gate_recv.at[t, k], (f, target)).start()

    def across(t, k, recv_x, recv_y):
        remote(unit(t, f, k), send_sem.at[t], recv_x.at[t], (fx, z)).start()
        remote(unit(t, f, k), send_sem.at[t], recv_y.at[t], (fy, z)).start()

    def diagonal(t, k, target):
        remote(unit(t, fd, k), send_sem.at[t], d_recv.at[t, k], (f, target)).start()

    def arrived(t, k):
        remote(unit(t, f, k), send_sem.at[t], z_recv.at[t, k], (f, z)).wait_recv()

        @pl.when(t < gate_steps)
        def _():
            remote(gate_of(t, k), gate_send.at[t], gate_recv.at[t, k], (f, z)).wait_recv()

    def own_first(t):
        @pl.when(z > 0)
        def _():
            along_z(t, z, z - 1)

        @pl.when(z < last)
        def _():
            along_z(t, z, z + 1)

        across(t, z, x_own, y_own)

    def z_hop(t, distance):
        @pl.when(z >= distance)
        def _():
            arrived(t, z - distance)

            @pl.when(z < last)
            def _():
                along_z(t, z - distance, z + 1)

            across(t, z - distance, x_rest, y_rest)

        @pl.when(z + distance < nz)
        def _():
            arrived(t, z + distance)

            @pl.when(z > 0)
            def _():
                along_z(t, z + distance, z - 1)

            across(t, z + distance, x_rest, y_rest)

    def line_done(t):
        remote(whole_line(t, f), core_send.at[t], core_recv.at[t], (fc, z)).start()

        @pl.when(t < gate_steps)
        def _():
            for k in range(nz):
                @pl.when(z != k)
                def _():
                    remote(gate_of(t, k), gate_core_send.at[t], gate_core_recv.at[t], (fc, z)).start()

    def gate_done(t):
        @pl.when(t < gate_steps)
        def _():
            others = table_ref.at[pl.ds(0, last * piece)]
            pltpu.make_async_copy(others, others, gate_core_recv.at[t]).wait()

    def plane(t):
        remote(unit(t, fx, z), send_sem.at[t], x_own.at[t], (fx, z)).wait_recv()
        remote(unit(t, fx, z, 0, half), send_sem.at[t], near_y.at[t], (fy, z)).start()
        remote(unit(t, fy, z), send_sem.at[t], y_own.at[t], (fy, z)).wait_recv()
        remote(unit(t, fy, z, half, half), send_sem.at[t], near_x.at[t], (fx, z)).start()

    def corner(t):
        remote(unit(t, fd, z, 0, half), send_sem.at[t], near_y.at[t], (fy, z)).wait_recv()
        remote(unit(t, fd, z, half, half), send_sem.at[t], near_x.at[t], (fx, z)).wait_recv()

        @pl.when(z > 0)
        def _():
            diagonal(t, z, z - 1)

        @pl.when(z < last)
        def _():
            diagonal(t, z, z + 1)

    def d_hop(t, distance):
        free = (t >= split) | (distance < reach)
        onward = (t >= split) | (distance + 1 < reach)

        @pl.when((z >= distance) & (free | (z < last)))
        def _():
            remote(unit(t, fd, z - distance), send_sem.at[t], d_recv.at[t, z - distance], (f, z)).wait_recv()

            if distance < reach:
                @pl.when((z < last) & (onward | (z + 1 < last)))
                def _():
                    diagonal(t, z - distance, z + 1)

        @pl.when((z + distance < nz) & (free | (z > 0)))
        def _():
            remote(unit(t, fd, z + distance), send_sem.at[t], d_recv.at[t, z + distance], (f, z)).wait_recv()

            if distance < reach:
                @pl.when((z > 0) & (onward | (z - 1 > 0)))
                def _():
                    diagonal(t, z + distance, z - 1)

    far = last - z
    middle = jnp.where(z == 0, reach, 1)

    def sides(t):
        rest = w_ref.at[t, pl.ds(0, last * shard)]
        remote(rest, send_sem.at[t], x_rest.at[t], (fx, z)).wait_recv()
        remote(rest, send_sem.at[t], y_rest.at[t], (fy, z)).wait_recv()

        @pl.when(at_end & (t < split))
        def _():
            remote(unit(t, fx, far), send_sem.at[t], far_y.at[t], (fy, z)).start()
            remote(unit(t, fy, middle), send_sem.at[t], far_x.at[t], (fx, z)).start()

        @pl.when(at_end & (t >= split))
        def _():
            remote(unit(t, fx, far, 0, half), send_sem.at[t], far_y.at[t], (fy, z)).start()
            remote(unit(t, fy, far, half, half), send_sem.at[t], far_x.at[t], (fx, z)).start()

        remote(whole_line(t, fx), core_send.at[t], core_recv.at[t], (fc, z)).start()
        remote(whole_line(t, fy), core_send.at[t], core_recv.at[t], (fc, z)).start()

    def corner_done(t):
        @pl.when(at_end & (t < split))
        def _():
            remote(unit(t, fd, far), send_sem.at[t], far_y.at[t], (fy, z)).wait_recv()
            remote(unit(t, fd, middle), send_sem.at[t], far_x.at[t], (fx, z)).wait_recv()

        @pl.when(at_end & (t >= split))
        def _():
            remote(unit(t, fd, far, 0, half), send_sem.at[t], far_y.at[t], (fy, z)).wait_recv()
            remote(unit(t, fd, far, half, half), send_sem.at[t], far_x.at[t], (fx, z)).wait_recv()

        remote(whole_line(t, fd), core_send.at[t], core_recv.at[t], (fc, z)).start()

    def multiply(t):
        whole = w_ref.at[t, pl.ds(0, 4 * line)]
        pltpu.make_async_copy(whole, whole, core_recv.at[t]).wait()
        blocks = normed_ref.shape[0] // 512
        column = pl.ds(pl.multiple_of((t % split) * LANES, LANES), LANES)

        def body(i, _):
            at = pl.ds(pl.multiple_of(i * 512, 512), 512)
            product = jnp.dot(normed_ref[at, :], w_ref[t], preferred_element_type=jnp.float32)

            @pl.when(t < split)
            def _():
                rec_ref[at, column] = product.astype(jnp.bfloat16)

            @pl.when(t >= split)
            def _():
                chunk = jnp.maximum(t - split, 0)
                state = b_ref[chunk, at, :] + a_ref[chunk, at, :] * start_ref[0:1, column]
                out_ref[at, column] = (state * jax.nn.gelu(product, approximate=True)).astype(out_ref.dtype)

            return 0

        lax.fori_loop(0, blocks, body, 0)

    def columns(h):
        return pl.ds(pl.multiple_of(h * channels, channels), channels)

    def tail_copy(h, source_rows, device):
        return pltpu.make_async_remote_copy(
            src_ref=rec_ref.at[pl.ds(source_rows, lead), columns(h)],
            dst_ref=before_ref.at[:, columns(h)],
            send_sem=tail_send.at[h], recv_sem=tail_recv.at[h],
            device_id=device, device_id_type=MESH,
        )

    def carry_copy(h, device):
        return pltpu.make_async_remote_copy(
            src_ref=carry_ref.at[:, columns(h)], dst_ref=start_ref.at[:, columns(h)],
            send_sem=carry_send.at[h], recv_sem=carry_recv.at[h],
            device_id=device, device_id_type=MESH,
        )

    def send_tail(h):
        @pl.when(z < last)
        def _():
            tail_copy(h, rows - lead, (f, z + 1)).start()

    def scan(h):
        @pl.when(z > 0)
        def _():
            tail_copy(h, rows - lead, (f, z)).wait_recv()

        cols = columns(h)
        padded_ref[pl.ds(0, lead), :] = before_ref[:, cols].astype(jnp.float32)
        padded_ref[pl.ds(lead, rows), :] = rec_ref[:, cols].astype(jnp.float32)
        conv_sum = jnp.zeros((rows, channels), jnp.float32) + bias_ref[:, cols]
        for tap in range(taps):
            conv_sum = conv_sum + weight_ref[tap : tap + 1, cols] * padded_ref[pl.ds(lead - tap, rows), :]
        conv_out = conv_sum.astype(jnp.bfloat16)
        gates = jnp.dot(conv_out, table_ref[cols, :], preferred_element_type=jnp.float32)
        input_gate = jax.nn.sigmoid(gates[:, :channels] + gate_bias_ref[0:1, cols])
        recur_gate = jax.nn.sigmoid(gates[:, channels:] + gate_bias_ref[1:2, cols])
        param = decay_ref[:, cols]
        softplus = jnp.maximum(param, 0.0) + jnp.log1p(jnp.exp(-jnp.abs(param)))
        log_decay = -8.0 * softplus * recur_gate
        decay = jnp.exp(log_decay)
        lost = -jnp.tanh(log_decay) * (decay * decay + 1.0)
        driven = jnp.sqrt(lost) * input_gate * conv_out.astype(jnp.float32)
        for j in range(pieces):
            a_ref[h * pieces + j] = decay[:, j * LANES : (j + 1) * LANES]
            b_ref[h * pieces + j] = driven[:, j * LANES : (j + 1) * LANES]

        lanes = 8
        length = rows // lanes

        def body(i, carry):
            at = pl.ds(i, lanes, stride=length)
            after = []
            for j in range(pieces):
                product, state = carry[j]
                decay_now = a_ref[h * pieces + j, at, :]
                product = product * decay_now
                state = decay_now * state + b_ref[h * pieces + j, at, :]
                a_ref[h * pieces + j, at, :] = product
                b_ref[h * pieces + j, at, :] = state
                after.append((product, state))
            return tuple(after)

        fresh = (jnp.ones((lanes, LANES), jnp.float32), jnp.zeros((lanes, LANES), jnp.float32))
        totals = lax.fori_loop(0, length, body, (fresh,) * pieces, unroll=8)
        for j in range(pieces):
            product, state = totals[j]
            start = jnp.zeros((1, LANES), jnp.float32)
            prefix = jnp.ones((1, LANES), jnp.float32)
            for i in range(lanes):
                at = pl.ds(i * length, length)
                within = a_ref[h * pieces + j, at, :]
                b_ref[h * pieces + j, at, :] = b_ref[h * pieces + j, at, :] + within * start
                a_ref[h * pieces + j, at, :] = within * prefix
                start = product[i : i + 1, :] * start + state[i : i + 1, :]
                prefix = prefix * product[i : i + 1, :]
            col = pl.ds(pl.multiple_of((h * pieces + j) * LANES, LANES), LANES)
            end_ref[0:1, col] = prefix
            end_ref[1:2, col] = start

    def make_carry(h):
        cols = columns(h)

        @pl.when(z > 0)
        def _():
            carry_copy(h, (f, z)).wait_recv()

        @pl.when(z < last)
        def _():
            end = end_ref[0:1, cols] * start_ref[0:1, cols] + end_ref[1:2, cols]
            carry_ref[:, cols] = jnp.broadcast_to(end, (carry_ref.shape[0], channels))

    def send_carry(h):
        @pl.when(z < last)
        def _():
            carry_copy(h, (f, z + 1)).start()

    @pl.when(z == 0)
    def _():
        before_ref[...] = jnp.zeros_like(before_ref)
        start_ref[...] = jnp.zeros_like(start_ref)

    stages = []
    for distance in range(1, nz):
        stages.append((functools.partial(z_hop, distance=distance), LEAD + GAP * (distance - 1)))
    stages += [(plane, LEAD), (corner, LEAD + GAP)]
    for distance in range(1, nz - 1):
        stages.append((functools.partial(d_hop, distance=distance), LEAD + GAP * (distance + 1)))
    line_lag = LEAD + GAP * (nz - 2)
    sides_lag = line_lag + GAP
    stages += [
        (line_done, line_lag), (gate_done, line_lag + 1),
        (sides, sides_lag), (corner_done, sides_lag + GAP), (own_first, 0),
    ]
    finish = sides_lag + GAP + 1
    tail_at = finish + pieces
    scan_at = max(tail_at + 2, line_lag + gate_steps)
    steps = chunks + finish

    def on_head(s, first, stage):
        @pl.when((s >= first) & (s < first + pieces * heads) & ((s - first) % pieces == 0))
        def _():
            stage((s - first) // pieces)

    def step(s, _):
        for stage, lag in stages:
            @pl.when((s >= lag) & (s < chunks + lag))
            def _():
                stage(s - lag)

        on_head(s, scan_at + 2 + 2 * z, send_carry)
        on_head(s, tail_at, send_tail)

        @pl.when(s == LEAD)
        def _():
            token_copy.wait()

        @pl.when((s >= LEAD) & (s < LEAD + NORM_PARTS))
        def _():
            normalise(normed_ref, gain_ref, s - LEAD, NORM_PARTS)

        on_head(s, scan_at + 1 + 2 * z, make_carry)

        @pl.when((s >= finish) & (s < chunks + finish))
        def _():
            multiply(s - finish)

        on_head(s, scan_at, scan)
        return 0

    lax.fori_loop(0, steps, step, 0)

    def units_sent(k, early):
        count = 2 + 2 * last + 1 + 2 * (int(k > 0) + int(k < last))
        for distance in range(1, nz):
            count += int(k >= distance and k < last) + int(k + distance < nz and k > 0)
            if distance < reach:
                open_up = not early or distance + 1 < reach or k + 1 < last
                open_down = not early or distance + 1 < reach or k - 1 > 0
                count += int(k >= distance and k < last and open_up)
                count += int(k + distance < nz and k > 0 and open_down)
        if k == 0 or k == last:
            count += 2 if early else 1
        return count

    def drain(t, _):
        for k in range(nz):
            passed = int(k > 0) + int(k < last)
            for distance in range(1, nz):
                passed += int(k >= distance and k < last) + int(k + distance < nz and k > 0)

            @pl.when(z == k)
            def _():
                for early in (True, False):
                    @pl.when((t < split) if early else (t >= split))
                    def _():
                        sent = w_ref.at[t, pl.ds(0, units_sent(k, early) * shard)]
                        pltpu.make_async_copy(sent, sent, send_sem.at[t]).wait()

                @pl.when(t < gate_steps)
                def _():
                    sent_gate = table_ref.at[pl.ds(0, passed * piece)]
                    pltpu.make_async_copy(sent_gate, sent_gate, gate_send.at[t]).wait()

        whole = w_ref.at[t, pl.ds(0, 4 * line)]
        pltpu.make_async_copy(whole, whole, core_send.at[t]).wait()

        @pl.when(t < gate_steps)
        def _():
            others = table_ref.at[pl.ds(0, last * piece)]
            pltpu.make_async_copy(others, others, gate_core_send.at[t]).wait()

        @pl.when((t < heads) & (z < last))
        def _():
            tail_copy(t, rows - lead, (f, z)).wait_send()
            carry_copy(t, (f, z)).wait_send()

        return 0

    lax.fori_loop(0, chunks, drain, 0)


def fused_branch(
    nz, tokens, norm_gain, lru_proj, gelu_proj, conv_weight, conv_bias, gate_weights, gate_bias,
    decay_param,
):
    rows, width = tokens.shape
    inner = lru_proj.shape[1]
    chunks = 2 * inner // LANES
    channels = gate_weights.shape[1] // 2
    heads = inner // channels
    vmem = pl.BlockSpec(memory_space=pltpu.VMEM)
    any_ = pl.BlockSpec(memory_space=pl.ANY)
    dma = pltpu.SemaphoreType.DMA
    f32, bf16 = jnp.float32, jnp.bfloat16
    lead = 16
    each = dma((chunks,))
    return pl.pallas_call(
        functools.partial(branch_kernel, nz),
        out_shape=jax.ShapeDtypeStruct((rows, inner), bf16),
        in_specs=[any_, vmem, any_, any_, any_, vmem, vmem, vmem, vmem],
        out_specs=vmem,
        scratch_shapes=[
            pltpu.VMEM((chunks, width, LANES), bf16),
            pltpu.VMEM((rows, width), bf16),
            pltpu.VMEM((rows, inner), bf16),
            pltpu.VMEM((gate_weights.shape[0] * nz, 2 * channels), bf16),
            pltpu.VMEM((lead, inner), bf16),
            pltpu.VMEM((lead + rows, channels), f32),
            pltpu.VMEM((chunks // 2, rows, LANES), f32),
            pltpu.VMEM((chunks // 2, rows, LANES), f32),
            pltpu.VMEM((8, inner), f32), pltpu.VMEM((8, inner), f32), pltpu.VMEM((8, inner), f32),
            dma((3,)), each, each, dma((chunks // 4,)), dma((chunks // 4,)),
            dma((heads,)), dma((heads,)),
            dma((chunks, nz)), dma((chunks, nz)), dma((chunks // 4, nz)), dma((chunks // 4,)),
            each, each, each, each, each, each, each, each, each,
            dma((heads,)), dma((heads,)),
        ],
        compiler_params=pltpu.CompilerParams(
            collective_id=0, has_side_effects=True, vmem_limit_bytes=VMEM_BYTES
        ),
    )(
        tokens, norm_gain.reshape(1, width), lru_proj, gelu_proj, gate_weights, conv_weight,
        conv_bias.reshape(1, inner), gate_bias, decay_param.reshape(1, inner),
    )


def scan_kernel(
    rec_ref, before_ref, weight_ref, bias_ref, table_ref, gate_bias_ref, decay_ref,
    state_ref, cumulative_ref, end_ref, padded_ref, a_ref, b_ref,
):
    rows, channels = rec_ref.shape
    taps = weight_ref.shape[0]
    lead = before_ref.shape[0]
    padded_ref[pl.ds(0, lead), :] = before_ref[...].astype(jnp.float32)
    padded_ref[pl.ds(lead, rows), :] = rec_ref[...].astype(jnp.float32)
    conv_sum = jnp.zeros((rows, channels), jnp.float32) + bias_ref[...]
    for tap in range(taps):
        conv_sum = conv_sum + weight_ref[tap : tap + 1, :] * padded_ref[pl.ds(lead - tap, rows), :]
    conv_out = conv_sum.astype(jnp.bfloat16)
    gates = jnp.dot(conv_out, table_ref[...], preferred_element_type=jnp.float32)
    input_gate = jax.nn.sigmoid(gates[:, :channels] + gate_bias_ref[0:1, :])
    recur_gate = jax.nn.sigmoid(gates[:, channels:] + gate_bias_ref[1:2, :])
    param = decay_ref[...]
    softplus = jnp.maximum(param, 0.0) + jnp.log1p(jnp.exp(-jnp.abs(param)))
    log_decay = -8.0 * softplus * recur_gate
    decay = jnp.exp(log_decay)
    lost = -jnp.tanh(log_decay) * (decay * decay + 1.0)
    driven = jnp.sqrt(lost) * input_gate * conv_out.astype(jnp.float32)
    parts = channels // LANES
    for j in range(parts):
        a_ref[j] = decay[:, j * LANES : (j + 1) * LANES]
        b_ref[j] = driven[:, j * LANES : (j + 1) * LANES]

    lanes = 8
    length = rows // lanes

    def body(i, carry):
        at = pl.ds(i, lanes, stride=length)
        after = []
        for j in range(parts):
            product, state = carry[j]
            decay_now = a_ref[j, at, :]
            product = product * decay_now
            state = decay_now * state + b_ref[j, at, :]
            a_ref[j, at, :] = product
            b_ref[j, at, :] = state
            after.append((product, state))
        return tuple(after)

    fresh = (jnp.ones((lanes, LANES), jnp.float32), jnp.zeros((lanes, LANES), jnp.float32))
    totals = lax.fori_loop(0, length, body, (fresh,) * parts, unroll=8)
    for j in range(parts):
        product, state = totals[j]
        cols = slice(j * LANES, (j + 1) * LANES)
        start = jnp.zeros((1, LANES), jnp.float32)
        prefix = jnp.ones((1, LANES), jnp.float32)
        for i in range(lanes):
            at = pl.ds(i * length, length)
            within = a_ref[j, at, :]
            state_ref[at, cols] = b_ref[j, at, :] + within * start
            cumulative_ref[at, cols] = within * prefix
            start = product[i : i + 1, :] * start + state[i : i + 1, :]
            prefix = prefix * product[i : i + 1, :]
        end_ref[0:1, cols] = prefix
        end_ref[1:2, cols] = start


def local_scan(rec, before, conv_weight, conv_bias, table, gate_bias, decay_param):
    rows, inner = rec.shape
    width = table.shape[1] // 2
    lead = before.shape[0]

    def columns(height):
        return pl.BlockSpec((height, width), lambda h: (0, h))

    return pl.pallas_call(
        scan_kernel,
        grid=(inner // width,),
        out_shape=(
            jax.ShapeDtypeStruct((rows, inner), jnp.float32),
            jax.ShapeDtypeStruct((rows, inner), jnp.float32),
            jax.ShapeDtypeStruct((2, inner), jnp.float32),
        ),
        in_specs=[
            columns(rows), columns(lead), columns(conv_weight.shape[0]), columns(1),
            pl.BlockSpec((width, 2 * width), lambda h: (h, 0)), columns(2), columns(1),
        ],
        out_specs=(columns(rows), columns(rows), columns(2)),
        scratch_shapes=[
            pltpu.VMEM((rows + lead, width), jnp.float32),
            pltpu.VMEM((width // LANES, rows, LANES), jnp.float32),
            pltpu.VMEM((width // LANES, rows, LANES), jnp.float32),
        ],
    )(
        rec, before, conv_weight, conv_bias.reshape(1, inner), table, gate_bias,
        decay_param.reshape(1, inner),
    )


def shards(
    nz, paired, tokens, norm_gain, lru_proj, gelu_proj, conv_weight, conv_bias, gate_weights,
    gate_bias, decay_param,
):
    seq_count, tok_rows, width = tokens.shape
    inner = lru_proj.shape[1]
    taps = conv_weight.shape[0]
    if paired:
        out = fused_branch(
            nz, tokens.reshape(tok_rows, width), norm_gain, lru_proj, gelu_proj, conv_weight,
            conv_bias, gate_weights, gate_bias, decay_param,
        )
        return out.reshape(seq_count, tok_rows, inner)
    flat = tokens.reshape(tok_rows, width).astype(jnp.float32)
    mean_square = jnp.mean(flat * flat, axis=-1, keepdims=True)
    normed = (flat * lax.rsqrt(mean_square + 1e-06) * norm_gain).astype(jnp.bfloat16)
    every = [
        lax.all_gather(w, ("fsdp", "seq"), axis=0, tiled=True) for w in (lru_proj, gelu_proj)
    ]
    rec = jnp.dot(normed, every[0], preferred_element_type=jnp.float32).astype(jnp.bfloat16)
    act = jnp.dot(normed, every[1], preferred_element_type=jnp.float32)
    table = lax.all_gather(gate_weights, "seq", axis=0, tiled=True)
    lead = 8
    before = lax.ppermute(
        rec[tok_rows - lead :, :], "seq", [(i, i + 1) for i in range(nz - 1)]
    )
    local, cumulative, ends = local_scan(
        rec, before, conv_weight, conv_bias, table, gate_bias, decay_param
    )
    every_end = lax.all_gather(ends, "seq")
    position = lax.axis_index("seq")
    start = jnp.zeros((inner,), jnp.float32)
    for k in range(nz - 1):
        start = jnp.where(k < position, every_end[k, 0] * start + every_end[k, 1], start)
    gelu = jax.nn.gelu(act, approximate=True)
    out = ((local + cumulative * start) * gelu).astype(jnp.bfloat16)
    return out.reshape(seq_count, tok_rows, inner)


def solution(mesh):
    placed = (
        P("fsdp", "seq", None), P(), P(("fsdp", "seq"), None), P(("fsdp", "seq"), None), P(), P(),
        P("seq", None), P(), P(),
    )
    nz = mesh.shape["seq"]
    paired = mesh.shape["fsdp"] == 8 and 3 < nz <= 5
    return jax.shard_map(
        functools.partial(shards, nz, paired), mesh=mesh, in_specs=placed,
        out_specs=P("fsdp", "seq", None), check_vma=False,
    )
```

```python
import functools

import jax
import jax.numpy as jnp
from jax import lax
from jax.experimental import pallas as pl
from jax.experimental.pallas import tpu as pltpu
from jax.sharding import PartitionSpec as P

MESH = pl.DeviceIdType.MESH
LANES = 128
VMEM_BYTES = 66_000_000


def normalise(normed_ref, gain_ref, part, parts):
    rows = 32

    def body(i, _):
        at = pl.ds(pl.multiple_of(i * rows, rows), rows)
        values = normed_ref[at, :].astype(jnp.float32)
        mean_square = jnp.mean(values * values, axis=-1, keepdims=True)
        normed_ref[at, :] = (values * lax.rsqrt(mean_square + 1e-06) * gain_ref[...]).astype(jnp.bfloat16)
        return 0

    blocks = normed_ref.shape[0] // rows // parts
    lax.fori_loop(part * blocks, (part + 1) * blocks, body, 0)


LEAD = 4
GAP = 2
NORM_PARTS = 4
TALL = 512


def hop_counts(nz, k, early, gates):
    last, reach = nz - 1, nz - 2
    twice = 2 if gates else 1
    end = k in (0, last)
    got = {0: 2, 1: 1}
    for distance in range(1, nz):
        sources = int(k >= distance) + int(k + distance < nz)
        got[distance - 1] = got.get(distance - 1, 0) + twice * sources
        if distance <= reach:
            for source in (k - distance, k + distance):
                if 0 <= source < nz and not (early and end and distance == reach):
                    got[distance + 1] = got.get(distance + 1, 0) + 1
    got[last] = got.get(last, 0) + 2 * last
    far = (2 if early else 1) if end else 0
    sent = 2 + 2 * last + 1 + far
    for source in range(nz):
        for target in (k - 1, k + 1):
            onward = (target - k) * (k - source) >= 0
            if not (0 <= target < nz and onward):
                continue
            sent += 1
            distance = abs(target - source)
            closed = early and target in (0, last) and distance == reach
            if distance <= reach and not closed:
                sent += 1
    passed = sum(
        1 for source in range(nz) for target in (k - 1, k + 1)
        if 0 <= target < nz and (target - k) * (k - source) >= 0
    )
    return got, far, sent, passed


def branch_kernel(
    nz,
    tokens_ref, gain_in, lru_ref, gelu_ref, gate_ref,
    weight_in, bias_in, gate_bias_in, decay_in,
    result_ref,
    gain_ref, weight_ref, bias_ref, gate_bias_ref, decay_ref, out_ref,
    w_ref, normed_ref, rec_ref, table_ref, before_ref, padded_ref, a_ref, b_ref,
    end_ref, carry_ref, start_ref,
    own_sem, out_sem, send_sem, core_send, gate_send, gate_core_send, tail_send, carry_send,
    hop_recv, far_recv, core_recv, gate_core_recv, tail_recv, carry_recv,
):
    f = lax.axis_index("fsdp")
    z = lax.axis_index("seq")
    c, x, y = f % 2, (f // 2) % 2, f // 4
    fx, fy, fc = f + 2 - 4 * x, f + 4 - 8 * y, f + 1 - 2 * c
    fd = fx + 4 - 8 * y
    shard = lru_ref.shape[0]
    line = shard * nz
    half = shard // 2
    chunks, _, wide = w_ref.shape
    split = chunks // 2
    gate_rows = gate_ref.shape[0]
    gate_steps = split // 2
    piece = gate_rows // 2 // gate_steps
    rows = normed_ref.shape[0]
    channels = table_ref.shape[1] // 2
    heads = rec_ref.shape[1] // channels
    pieces = channels // LANES
    taps = weight_ref.shape[0]
    lead = before_ref.shape[0]
    last = nz - 1
    reach = nz - 2
    at_end = (z == 0) | (z == last)

    def remote(src, send, recv, device):
        return pltpu.make_async_remote_copy(
            src_ref=src, dst_ref=src, send_sem=send, recv_sem=recv,
            device_id=device, device_id_type=MESH,
        )

    own = pl.ds(pl.multiple_of((f * nz + z) * shard, shard), shard)
    for t in range(chunks):
        src = lru_ref if t < split else gelu_ref
        cols = pl.ds((t % split) * wide, wide)
        pltpu.make_async_copy(src.at[:, cols], w_ref.at[t, own], own_sem.at[0]).start()
    own_gate = pl.ds(pl.multiple_of(z * gate_rows, gate_rows), gate_rows)
    gate_copy = pltpu.make_async_copy(gate_ref, table_ref.at[own_gate], own_sem.at[1])
    gate_copy.start()
    token_copy = pltpu.make_async_copy(tokens_ref, normed_ref, own_sem.at[2])
    token_copy.start()
    small = [
        pltpu.make_async_copy(source, target, own_sem.at[3 + i])
        for i, (source, target) in enumerate((
            (gain_in, gain_ref), (weight_in, weight_ref), (bias_in, bias_ref),
            (gate_bias_in, gate_bias_ref), (decay_in, decay_ref),
        ))
    ]
    for copy in small:
        copy.start()

    barrier = pltpu.get_barrier_semaphore()
    for device in ((fx, z), (fy, z), (fc, z)):
        pl.semaphore_signal(barrier, inc=1, device_id=device, device_id_type=MESH)

    @pl.when(z > 0)
    def _():
        pl.semaphore_signal(barrier, inc=1, device_id=(f, z - 1), device_id_type=MESH)

    @pl.when(z < last)
    def _():
        pl.semaphore_signal(barrier, inc=1, device_id=(f, z + 1), device_id_type=MESH)

    for k in range(nz):
        @pl.when(z == k)
        def _():
            pl.semaphore_wait(barrier, 3 + int(k > 0) + int(k < last))

    pltpu.make_async_copy(w_ref.at[:, own], w_ref.at[:, own], own_sem.at[0]).wait()
    gate_copy.wait()

    def unit(t, owner, k, first=0, size=shard):
        start = (owner * nz + k) * shard + first
        return w_ref.at[t, pl.ds(pl.multiple_of(start, half), size)]

    def whole_line(t, owner):
        return w_ref.at[t, pl.ds(pl.multiple_of(owner * line, line), line)]

    def gate_of(t, source):
        first = source * gate_rows + c * (gate_rows // 2) + t * piece
        return table_ref.at[pl.ds(pl.multiple_of(first, piece), piece)]

    send, core = send_sem.at[0], core_send.at[0]

    def along_z(t, k, target, distance):
        remote(unit(t, f, k), send, hop_recv.at[t, distance - 1], (f, target)).start()

        @pl.when(t < gate_steps)
        def _():
            remote(gate_of(t, k), gate_send.at[0], hop_recv.at[t, distance - 1], (f, target)).start()

    def across(t, k, hop):
        remote(unit(t, f, k), send, hop_recv.at[t, hop], (fx, z)).start()
        remote(unit(t, f, k), send, hop_recv.at[t, hop], (fy, z)).start()

    def diagonal(t, k, target, distance):
        remote(unit(t, fd, k), send, hop_recv.at[t, distance + 1], (f, target)).start()

    def wait_hop(t, hop):
        sizes = {}
        for k in range(nz):
            for early, gates in ((True, True), (True, False), (False, False)):
                count = hop_counts(nz, k, early, gates)[0].get(hop, 0)
                sizes.setdefault(count, {}).setdefault((early, gates), []).append(k)
        for count, places in sizes.items():
            if count == 0:
                continue
            chosen = False
            for (early, gates), ks in places.items():
                when = (t < gate_steps) if gates else ((t >= gate_steps) & (t < split)) if early else (t >= split)
                if len(ks) < nz:
                    there = z == ks[0]
                    for k in ks[1:]:
                        there = there | (z == k)
                    when = when & there
                chosen = when if chosen is False else chosen | when

            @pl.when(chosen)
            def _():
                block = w_ref.at[0, pl.ds(0, count * shard)]
                pltpu.make_async_copy(block, block, hop_recv.at[t, hop]).wait()

    def own_first(t):
        @pl.when(z > 0)
        def _():
            along_z(t, z, z - 1, 1)

        @pl.when(z < last)
        def _():
            along_z(t, z, z + 1, 1)

        across(t, z, 0)

    def z_hop(t, distance):
        @pl.when((z >= distance) & (z < last))
        def _():
            along_z(t, z - distance, z + 1, distance + 1)

        @pl.when((z + distance < nz) & (z > 0))
        def _():
            along_z(t, z + distance, z - 1, distance + 1)

    def sideways(t, distance):
        @pl.when(z >= distance)
        def _():
            across(t, z - distance, last)

        @pl.when(z + distance < nz)
        def _():
            across(t, z + distance, last)

    def d_hop(t, distance):
        onward = (t >= split) | (distance + 1 < reach)

        @pl.when((z >= distance) & (z < last) & (onward | (z + 1 < last)))
        def _():
            diagonal(t, z - distance, z + 1, distance + 1)

        @pl.when((z + distance < nz) & (z > 0) & (onward | (z - 1 > 0)))
        def _():
            diagonal(t, z + distance, z - 1, distance + 1)

    far = last - z
    middle = jnp.where(z == 0, reach, 1)

    def hop_done(t, hop):
        wait_hop(t, hop)
        if hop + 1 < last:
            z_hop(t, hop + 1)
        if hop == 0:
            remote(unit(t, fx, z, 0, half), send, hop_recv.at[t, 1], (fy, z)).start()
            remote(unit(t, fy, z, half, half), send, hop_recv.at[t, 1], (fx, z)).start()
        if hop == 1:
            @pl.when(z > 0)
            def _():
                diagonal(t, z, z - 1, 1)

            @pl.when(z < last)
            def _():
                diagonal(t, z, z + 1, 1)
        if 2 <= hop < last:
            d_hop(t, hop - 1)
        if hop + 1 <= last:
            sideways(t, hop + 1)
        if hop + 1 == last:
            remote(whole_line(t, f), core, core_recv.at[t], (fc, z)).start()

            @pl.when(t < gate_steps)
            def _():
                for k in range(nz):
                    @pl.when(z != k)
                    def _():
                        remote(gate_of(t, k), gate_core_send.at[0], gate_core_recv.at[t], (fc, z)).start()
        if hop == last:
            @pl.when(at_end & (t < split))
            def _():
                remote(unit(t, fx, far), send, far_recv.at[t], (fy, z)).start()
                remote(unit(t, fy, middle), send, far_recv.at[t], (fx, z)).start()

            @pl.when(at_end & (t >= split))
            def _():
                remote(unit(t, fx, far, 0, half), send, far_recv.at[t], (fy, z)).start()
                remote(unit(t, fy, far, half, half), send, far_recv.at[t], (fx, z)).start()

            remote(whole_line(t, fx), core, core_recv.at[t], (fc, z)).start()
            remote(whole_line(t, fy), core, core_recv.at[t], (fc, z)).start()

    def gate_done(t):
        @pl.when(t < gate_steps)
        def _():
            others = table_ref.at[pl.ds(0, last * piece)]
            pltpu.make_async_copy(others, others, gate_core_recv.at[t]).wait()

    def corner_done(t):
        @pl.when(at_end & (t < split))
        def _():
            block = w_ref.at[0, pl.ds(0, 2 * shard)]
            pltpu.make_async_copy(block, block, far_recv.at[t]).wait()

        @pl.when(at_end & (t >= split))
        def _():
            block = w_ref.at[0, pl.ds(0, shard)]
            pltpu.make_async_copy(block, block, far_recv.at[t]).wait()

        remote(whole_line(t, fd), core, core_recv.at[t], (fc, z)).start()

    def put_out(h):
        return pltpu.make_async_copy(out_ref.at[:, columns(h)], result_ref.at[:, columns(h)], out_sem.at[0])

    def multiply(t):
        whole = w_ref.at[t, pl.ds(0, 4 * line)]
        pltpu.make_async_copy(whole, whole, core_recv.at[t]).wait()
        column = columns(t % split)
        tall = TALL

        def body(i, _):
            at = pl.ds(pl.multiple_of(i * tall, tall), tall)
            product = jnp.dot(normed_ref[at, :], w_ref[t], preferred_element_type=jnp.float32)

            @pl.when(t < split)
            def _():
                rec_ref[at, column] = product.astype(jnp.bfloat16)

            @pl.when(t >= split)
            def _():
                h = jnp.maximum(t - split, 0)
                for j in range(pieces):
                    lanes = pl.ds(pl.multiple_of(h * channels + j * LANES, LANES), LANES)
                    state = b_ref[h * pieces + j, at, :] + a_ref[h * pieces + j, at, :] * start_ref[0:1, lanes]
                    act = jax.nn.gelu(product[:, j * LANES : (j + 1) * LANES], approximate=True)
                    out_ref[at, lanes] = (state * act).astype(out_ref.dtype)

            return 0

        lax.fori_loop(0, rows // tall, body, 0)

        @pl.when(t >= split)
        def _():
            put_out(t - split).start()

    def columns(h):
        return pl.ds(pl.multiple_of(h * channels, channels), channels)

    def tail_copy(h, source_rows, device):
        return pltpu.make_async_remote_copy(
            src_ref=rec_ref.at[pl.ds(source_rows, lead), columns(h)],
            dst_ref=before_ref.at[:, columns(h)],
            send_sem=tail_send.at[0], recv_sem=tail_recv.at[h],
            device_id=device, device_id_type=MESH,
        )

    def carry_copy(h, device):
        return pltpu.make_async_remote_copy(
            src_ref=carry_ref.at[:, columns(h)], dst_ref=start_ref.at[:, columns(h)],
            send_sem=carry_send.at[0], recv_sem=carry_recv.at[h],
            device_id=device, device_id_type=MESH,
        )

    def send_tail(h):
        @pl.when(z < last)
        def _():
            tail_copy(h, rows - lead, (f, z + 1)).start()

    def scan(h):
        @pl.when(z > 0)
        def _():
            tail_copy(h, rows - lead, (f, z)).wait_recv()

        cols = columns(h)
        padded_ref[pl.ds(0, lead), :] = before_ref[:, cols].astype(jnp.float32)
        padded_ref[pl.ds(lead, rows), :] = rec_ref[:, cols].astype(jnp.float32)
        conv_sum = jnp.zeros((rows, channels), jnp.float32) + bias_ref[:, cols]
        for tap in range(taps):
            conv_sum = conv_sum + weight_ref[tap : tap + 1, cols] * padded_ref[pl.ds(lead - tap, rows), :]
        conv_out = conv_sum.astype(jnp.bfloat16)
        gates = jnp.dot(conv_out, table_ref[cols, :], preferred_element_type=jnp.float32)
        input_gate = jax.nn.sigmoid(gates[:, :channels] + gate_bias_ref[0:1, cols])
        recur_gate = jax.nn.sigmoid(gates[:, channels:] + gate_bias_ref[1:2, cols])
        param = decay_ref[:, cols]
        softplus = jnp.maximum(param, 0.0) + jnp.log1p(jnp.exp(-jnp.abs(param)))
        log_decay = -8.0 * softplus * recur_gate
        decay = jnp.exp(log_decay)
        lost = -jnp.tanh(log_decay) * (decay * decay + 1.0)
        driven = jnp.sqrt(lost) * input_gate * conv_out.astype(jnp.float32)
        for j in range(pieces):
            a_ref[h * pieces + j] = decay[:, j * LANES : (j + 1) * LANES]
            b_ref[h * pieces + j] = driven[:, j * LANES : (j + 1) * LANES]

        lanes = 8
        length = rows // lanes

        def body(i, carry):
            at = pl.ds(i, lanes, stride=length)
            after = []
            for j in range(pieces):
                product, state = carry[j]
                decay_now = a_ref[h * pieces + j, at, :]
                product = product * decay_now
                state = decay_now * state + b_ref[h * pieces + j, at, :]
                a_ref[h * pieces + j, at, :] = product
                b_ref[h * pieces + j, at, :] = state
                after.append((product, state))
            return tuple(after)

        fresh = (jnp.ones((lanes, LANES), jnp.float32), jnp.zeros((lanes, LANES), jnp.float32))
        totals = lax.fori_loop(0, length, body, (fresh,) * pieces, unroll=8)
        for j in range(pieces):
            product, state = totals[j]
            start = jnp.zeros((1, LANES), jnp.float32)
            prefix = jnp.ones((1, LANES), jnp.float32)
            for i in range(lanes):
                at = pl.ds(i * length, length)
                within = a_ref[h * pieces + j, at, :]
                b_ref[h * pieces + j, at, :] = b_ref[h * pieces + j, at, :] + within * start
                a_ref[h * pieces + j, at, :] = within * prefix
                start = product[i : i + 1, :] * start + state[i : i + 1, :]
                prefix = prefix * product[i : i + 1, :]
            col = pl.ds(pl.multiple_of((h * pieces + j) * LANES, LANES), LANES)
            end_ref[0:1, col] = prefix
            end_ref[1:2, col] = start

    def make_carry(h):
        cols = columns(h)

        @pl.when(z > 0)
        def _():
            carry_copy(h, (f, z)).wait_recv()

        @pl.when(z < last)
        def _():
            end = end_ref[0:1, cols] * start_ref[0:1, cols] + end_ref[1:2, cols]
            carry_ref[:, cols] = jnp.broadcast_to(end, (carry_ref.shape[0], channels))

    def send_carry(h):
        @pl.when(z < last)
        def _():
            carry_copy(h, (f, z + 1)).start()

    @pl.when(z == 0)
    def _():
        before_ref[...] = jnp.zeros_like(before_ref)
        start_ref[...] = jnp.zeros_like(start_ref)

    stages = []
    for hop in range(nz):
        stages.append((functools.partial(hop_done, hop=hop), LEAD + GAP * hop))
    line_lag = LEAD + GAP * reach
    sides_lag = LEAD + GAP * last
    stages += [(gate_done, line_lag + 1), (corner_done, sides_lag + GAP), (own_first, 0)]
    finish = sides_lag + GAP + 1
    tail_at = finish + 1
    scan_at = max(tail_at + 1, line_lag + gate_steps)
    steps = chunks + finish

    def on_head(s, first, stage):
        @pl.when((s >= first) & (s < first + heads))
        def _():
            stage(s - first)

    def step(s, _):
        for stage, lag in stages:
            @pl.when((s >= lag) & (s < chunks + lag))
            def _():
                stage(s - lag)

        on_head(s, scan_at + 2 + z, send_carry)
        on_head(s, tail_at, send_tail)

        @pl.when(s == LEAD)
        def _():
            token_copy.wait()
            for copy in small:
                copy.wait()

        @pl.when((s >= LEAD) & (s < LEAD + NORM_PARTS))
        def _():
            normalise(normed_ref, gain_ref, s - LEAD, NORM_PARTS)

        @pl.when((s >= finish) & (s < chunks + finish))
        def _():
            multiply(s - finish)

        on_head(s, scan_at, scan)
        on_head(s, scan_at + 1 + z, make_carry)
        return 0

    lax.fori_loop(0, steps, step, 0)

    for k in range(nz):
        early, late = hop_counts(nz, k, True, False), hop_counts(nz, k, False, False)

        @pl.when(z == k)
        def _():
            total = split * (early[2] + late[2])
            deep = max(n for n in range(1, chunks + 1) if total % n == 0)
            sent = w_ref.at[pl.ds(0, deep), pl.ds(0, total // deep * shard)]
            pltpu.make_async_copy(sent, sent, send).wait()
            sent_gate = table_ref.at[pl.ds(0, early[3] * piece * gate_steps)]
            pltpu.make_async_copy(sent_gate, sent_gate, gate_send.at[0]).wait()

    whole = w_ref.at[:, pl.ds(0, 4 * line)]
    pltpu.make_async_copy(whole, whole, core).wait()
    others = table_ref.at[pl.ds(0, last * piece * gate_steps)]
    pltpu.make_async_copy(others, others, gate_core_send.at[0]).wait()
    pltpu.make_async_copy(out_ref, result_ref, out_sem.at[0]).wait()

    @pl.when(z < last)
    def _():
        pltpu.make_async_copy(before_ref, before_ref, tail_send.at[0]).wait()
        pltpu.make_async_copy(carry_ref, carry_ref, carry_send.at[0]).wait()


def fused_branch(
    nz, tokens, norm_gain, lru_proj, gelu_proj, conv_weight, conv_bias, gate_weights, gate_bias,
    decay_param,
):
    rows, width = tokens.shape
    inner = lru_proj.shape[1]
    channels = gate_weights.shape[1] // 2
    chunks = 2 * inner // channels
    heads = inner // channels
    any_ = pl.BlockSpec(memory_space=pl.ANY)
    dma = pltpu.SemaphoreType.DMA
    f32, bf16 = jnp.float32, jnp.bfloat16
    lead = 16
    return pl.pallas_call(
        functools.partial(branch_kernel, nz),
        out_shape=jax.ShapeDtypeStruct((rows, inner), bf16),
        in_specs=[any_] * 9,
        out_specs=any_,
        scratch_shapes=[
            pltpu.VMEM((1, width), f32), pltpu.VMEM(conv_weight.shape, f32), pltpu.VMEM((1, inner), f32),
            pltpu.VMEM(gate_bias.shape, f32), pltpu.VMEM((1, inner), f32), pltpu.VMEM((rows, inner), bf16),
            pltpu.VMEM((chunks, width, channels), bf16),
            pltpu.VMEM((rows, width), bf16),
            pltpu.VMEM((rows, inner), bf16),
            pltpu.VMEM((gate_weights.shape[0] * nz, 2 * channels), bf16),
            pltpu.VMEM((lead, inner), bf16),
            pltpu.VMEM((lead + rows, channels), f32),
            pltpu.VMEM((inner // LANES, rows, LANES), f32),
            pltpu.VMEM((inner // LANES, rows, LANES), f32),
            pltpu.VMEM((8, inner), f32), pltpu.VMEM((8, inner), f32), pltpu.VMEM((8, inner), f32),
            dma((8,)), dma((1,)), dma((1,)), dma((1,)), dma((1,)), dma((1,)), dma((1,)), dma((1,)),
            dma((chunks, nz)), dma((chunks,)), dma((chunks,)), dma((chunks // 4,)),
            dma((heads,)), dma((heads,)),
        ],
        compiler_params=pltpu.CompilerParams(
            collective_id=0, has_side_effects=True, vmem_limit_bytes=VMEM_BYTES
        ),
    )(
        tokens, norm_gain.reshape(1, width), lru_proj, gelu_proj, gate_weights, conv_weight,
        conv_bias.reshape(1, inner), gate_bias, decay_param.reshape(1, inner),
    )


def scan_kernel(
    rec_ref, before_ref, weight_ref, bias_ref, table_ref, gate_bias_ref, decay_ref,
    state_ref, cumulative_ref, end_ref, padded_ref, a_ref, b_ref,
):
    rows, channels = rec_ref.shape
    taps = weight_ref.shape[0]
    lead = before_ref.shape[0]
    padded_ref[pl.ds(0, lead), :] = before_ref[...].astype(jnp.float32)
    padded_ref[pl.ds(lead, rows), :] = rec_ref[...].astype(jnp.float32)
    conv_sum = jnp.zeros((rows, channels), jnp.float32) + bias_ref[...]
    for tap in range(taps):
        conv_sum = conv_sum + weight_ref[tap : tap + 1, :] * padded_ref[pl.ds(lead - tap, rows), :]
    conv_out = conv_sum.astype(jnp.bfloat16)
    gates = jnp.dot(conv_out, table_ref[...], preferred_element_type=jnp.float32)
    input_gate = jax.nn.sigmoid(gates[:, :channels] + gate_bias_ref[0:1, :])
    recur_gate = jax.nn.sigmoid(gates[:, channels:] + gate_bias_ref[1:2, :])
    param = decay_ref[...]
    softplus = jnp.maximum(param, 0.0) + jnp.log1p(jnp.exp(-jnp.abs(param)))
    log_decay = -8.0 * softplus * recur_gate
    decay = jnp.exp(log_decay)
    lost = -jnp.tanh(log_decay) * (decay * decay + 1.0)
    driven = jnp.sqrt(lost) * input_gate * conv_out.astype(jnp.float32)
    parts = channels // LANES
    for j in range(parts):
        a_ref[j] = decay[:, j * LANES : (j + 1) * LANES]
        b_ref[j] = driven[:, j * LANES : (j + 1) * LANES]

    lanes = 8
    length = rows // lanes

    def body(i, carry):
        at = pl.ds(i, lanes, stride=length)
        after = []
        for j in range(parts):
            product, state = carry[j]
            decay_now = a_ref[j, at, :]
            product = product * decay_now
            state = decay_now * state + b_ref[j, at, :]
            a_ref[j, at, :] = product
            b_ref[j, at, :] = state
            after.append((product, state))
        return tuple(after)

    fresh = (jnp.ones((lanes, LANES), jnp.float32), jnp.zeros((lanes, LANES), jnp.float32))
    totals = lax.fori_loop(0, length, body, (fresh,) * parts, unroll=8)
    for j in range(parts):
        product, state = totals[j]
        cols = slice(j * LANES, (j + 1) * LANES)
        start = jnp.zeros((1, LANES), jnp.float32)
        prefix = jnp.ones((1, LANES), jnp.float32)
        for i in range(lanes):
            at = pl.ds(i * length, length)
            within = a_ref[j, at, :]
            state_ref[at, cols] = b_ref[j, at, :] + within * start
            cumulative_ref[at, cols] = within * prefix
            start = product[i : i + 1, :] * start + state[i : i + 1, :]
            prefix = prefix * product[i : i + 1, :]
        end_ref[0:1, cols] = prefix
        end_ref[1:2, cols] = start


def local_scan(rec, before, conv_weight, conv_bias, table, gate_bias, decay_param):
    rows, inner = rec.shape
    width = table.shape[1] // 2
    lead = before.shape[0]

    def columns(height):
        return pl.BlockSpec((height, width), lambda h: (0, h))

    return pl.pallas_call(
        scan_kernel,
        grid=(inner // width,),
        out_shape=(
            jax.ShapeDtypeStruct((rows, inner), jnp.float32),
            jax.ShapeDtypeStruct((rows, inner), jnp.float32),
            jax.ShapeDtypeStruct((2, inner), jnp.float32),
        ),
        in_specs=[
            columns(rows), columns(lead), columns(conv_weight.shape[0]), columns(1),
            pl.BlockSpec((width, 2 * width), lambda h: (h, 0)), columns(2), columns(1),
        ],
        out_specs=(columns(rows), columns(rows), columns(2)),
        scratch_shapes=[
            pltpu.VMEM((rows + lead, width), jnp.float32),
            pltpu.VMEM((width // LANES, rows, LANES), jnp.float32),
            pltpu.VMEM((width // LANES, rows, LANES), jnp.float32),
        ],
    )(
        rec, before, conv_weight, conv_bias.reshape(1, inner), table, gate_bias,
        decay_param.reshape(1, inner),
    )


def shards(
    nz, paired, tokens, norm_gain, lru_proj, gelu_proj, conv_weight, conv_bias, gate_weights,
    gate_bias, decay_param,
):
    seq_count, tok_rows, width = tokens.shape
    inner = lru_proj.shape[1]
    taps = conv_weight.shape[0]
    if paired:
        out = fused_branch(
            nz, tokens.reshape(tok_rows, width), norm_gain, lru_proj, gelu_proj, conv_weight,
            conv_bias, gate_weights, gate_bias, decay_param,
        )
        return out.reshape(seq_count, tok_rows, inner)
    flat = tokens.reshape(tok_rows, width).astype(jnp.float32)
    mean_square = jnp.mean(flat * flat, axis=-1, keepdims=True)
    normed = (flat * lax.rsqrt(mean_square + 1e-06) * norm_gain).astype(jnp.bfloat16)
    every = [
        lax.all_gather(w, ("fsdp", "seq"), axis=0, tiled=True) for w in (lru_proj, gelu_proj)
    ]
    rec = jnp.dot(normed, every[0], preferred_element_type=jnp.float32).astype(jnp.bfloat16)
    act = jnp.dot(normed, every[1], preferred_element_type=jnp.float32)
    table = lax.all_gather(gate_weights, "seq", axis=0, tiled=True)
    lead = 8
    before = lax.ppermute(
        rec[tok_rows - lead :, :], "seq", [(i, i + 1) for i in range(nz - 1)]
    )
    local, cumulative, ends = local_scan(
        rec, before, conv_weight, conv_bias, table, gate_bias, decay_param
    )
    every_end = lax.all_gather(ends, "seq")
    position = lax.axis_index("seq")
    start = jnp.zeros((inner,), jnp.float32)
    for k in range(nz - 1):
        start = jnp.where(k < position, every_end[k, 0] * start + every_end[k, 1], start)
    gelu = jax.nn.gelu(act, approximate=True)
    out = ((local + cumulative * start) * gelu).astype(jnp.bfloat16)
    return out.reshape(seq_count, tok_rows, inner)


def solution(mesh):
    placed = (
        P("fsdp", "seq", None), P(), P(("fsdp", "seq"), None), P(("fsdp", "seq"), None), P(), P(),
        P("seq", None), P(), P(),
    )
    nz = mesh.shape["seq"]
    paired = mesh.shape["fsdp"] == 8 and 3 < nz <= 5
    return jax.shard_map(
        functools.partial(shards, nz, paired), mesh=mesh, in_specs=placed,
        out_specs=P("fsdp", "seq", None), check_vma=False,
    )
```

```python
import functools

import jax
import jax.numpy as jnp
from jax import lax
from jax.experimental import pallas as pl
from jax.experimental.pallas import tpu as pltpu
from jax.sharding import PartitionSpec as P

MESH = pl.DeviceIdType.MESH
LANES = 128
VMEM_BYTES = 58_000_000


def normalise(normed_ref, gain_ref, part, parts):
    rows = 32

    def body(i, _):
        at = pl.ds(pl.multiple_of(i * rows, rows), rows)
        values = normed_ref[at, :].astype(jnp.float32)
        mean_square = jnp.mean(values * values, axis=-1, keepdims=True)
        normed_ref[at, :] = (values * lax.rsqrt(mean_square + 1e-06) * gain_ref[...]).astype(jnp.bfloat16)
        return 0

    blocks = normed_ref.shape[0] // rows // parts
    lax.fori_loop(part * blocks, (part + 1) * blocks, body, 0)


LAGS = (4, 7, 10, 12, 13)
NORM_PARTS = 4
TALL = 512


def hop_counts(nz, k, early, gates):
    last, reach = nz - 1, nz - 2
    twice = 2 if gates else 1
    end = k in (0, last)
    got = {0: 2, 1: 1}
    for distance in range(1, nz):
        sources = int(k >= distance) + int(k + distance < nz)
        got[distance - 1] = got.get(distance - 1, 0) + twice * sources
        if distance <= reach:
            for source in (k - distance, k + distance):
                if 0 <= source < nz and not (early and end and distance == reach):
                    got[distance + 1] = got.get(distance + 1, 0) + 1
    got[last] = got.get(last, 0) + 2 * last
    far = (2 if early else 1) if end else 0
    sent = 2 + 2 * last + 1 + far
    for source in range(nz):
        for target in (k - 1, k + 1):
            onward = (target - k) * (k - source) >= 0
            if not (0 <= target < nz and onward):
                continue
            sent += 1
            distance = abs(target - source)
            closed = early and target in (0, last) and distance == reach
            if distance <= reach and not closed:
                sent += 1
    passed = sum(
        1 for source in range(nz) for target in (k - 1, k + 1)
        if 0 <= target < nz and (target - k) * (k - source) >= 0
    )
    return got, far, sent, passed


def branch_kernel(
    nz,
    tokens_ref, gain_in, lru_ref, gelu_ref, gate_ref,
    weight_in, bias_in, gate_bias_in, decay_in,
    out_ref,
    gain_ref, weight_ref, bias_ref, gate_bias_ref, decay_ref,
    w_ref, normed_ref, rec_ref, table_ref, before_ref, padded_ref, a_ref, b_ref,
    end_ref, carry_ref, start_ref,
    own_sem, out_sem, send_sem, core_send, gate_send, gate_core_send, tail_send, carry_send,
    hop_recv, far_recv, core_recv, gate_core_recv, tail_recv, carry_recv,
):
    f = lax.axis_index("fsdp")
    z = lax.axis_index("seq")
    c, x, y = f % 2, (f // 2) % 2, f // 4
    fx, fy, fc = f + 2 - 4 * x, f + 4 - 8 * y, f + 1 - 2 * c
    fd = fx + 4 - 8 * y
    shard = lru_ref.shape[0]
    line = shard * nz
    half = shard // 2
    chunks, _, wide = w_ref.shape
    split = chunks // 2
    gate_rows = gate_ref.shape[0]
    gate_steps = split // 2
    piece = gate_rows // 2 // gate_steps
    rows = normed_ref.shape[0]
    channels = table_ref.shape[1] // 2
    heads = rec_ref.shape[1] // channels
    pieces = channels // LANES
    taps = weight_ref.shape[0]
    lead = before_ref.shape[0]
    last = nz - 1
    reach = nz - 2
    at_end = (z == 0) | (z == last)

    def remote(src, send, recv, device):
        return pltpu.make_async_remote_copy(
            src_ref=src, dst_ref=src, send_sem=send, recv_sem=recv,
            device_id=device, device_id_type=MESH,
        )

    own = pl.ds(pl.multiple_of((f * nz + z) * shard, shard), shard)
    for t in range(chunks):
        src = lru_ref if t < split else gelu_ref
        cols = pl.ds((t % split) * wide, wide)
        pltpu.make_async_copy(src.at[:, cols], w_ref.at[t, own], own_sem.at[0]).start()
    own_gate = pl.ds(pl.multiple_of(z * gate_rows, gate_rows), gate_rows)
    gate_copy = pltpu.make_async_copy(gate_ref, table_ref.at[own_gate], own_sem.at[1])
    gate_copy.start()
    token_copy = pltpu.make_async_copy(tokens_ref, normed_ref, own_sem.at[2])
    token_copy.start()
    small = [
        pltpu.make_async_copy(source, target, own_sem.at[3 + i])
        for i, (source, target) in enumerate((
            (gain_in, gain_ref), (weight_in, weight_ref), (bias_in, bias_ref),
            (gate_bias_in, gate_bias_ref), (decay_in, decay_ref),
        ))
    ]
    for copy in small:
        copy.start()

    barrier = pltpu.get_barrier_semaphore()
    for device in ((fx, z), (fy, z), (fc, z)):
        pl.semaphore_signal(barrier, inc=1, device_id=device, device_id_type=MESH)

    @pl.when(z > 0)
    def _():
        pl.semaphore_signal(barrier, inc=1, device_id=(f, z - 1), device_id_type=MESH)

    @pl.when(z < last)
    def _():
        pl.semaphore_signal(barrier, inc=1, device_id=(f, z + 1), device_id_type=MESH)

    for k in range(nz):
        @pl.when(z == k)
        def _():
            pl.semaphore_wait(barrier, 3 + int(k > 0) + int(k < last))

    pltpu.make_async_copy(w_ref.at[:, own], w_ref.at[:, own], own_sem.at[0]).wait()
    gate_copy.wait()

    def unit(t, owner, k, first=0, size=shard):
        start = (owner * nz + k) * shard + first
        return w_ref.at[t, pl.ds(pl.multiple_of(start, half), size)]

    def whole_line(t, owner):
        return w_ref.at[t, pl.ds(pl.multiple_of(owner * line, line), line)]

    def gate_of(t, source):
        first = source * gate_rows + c * (gate_rows // 2) + t * piece
        return table_ref.at[pl.ds(pl.multiple_of(first, piece), piece)]

    send, core = send_sem.at[0], core_send.at[0]

    def along_z(t, k, target, distance):
        remote(unit(t, f, k), send, hop_recv.at[t, distance - 1], (f, target)).start()

        @pl.when(t < gate_steps)
        def _():
            remote(gate_of(t, k), gate_send.at[0], hop_recv.at[t, distance - 1], (f, target)).start()

    def across(t, k, hop):
        remote(unit(t, f, k), send, hop_recv.at[t, hop], (fx, z)).start()
        remote(unit(t, f, k), send, hop_recv.at[t, hop], (fy, z)).start()

    def diagonal(t, k, target, distance):
        remote(unit(t, fd, k), send, hop_recv.at[t, distance + 1], (f, target)).start()

    def wait_hop(t, hop):
        sizes = {}
        for k in range(nz):
            for early, gates in ((True, True), (True, False), (False, False)):
                count = hop_counts(nz, k, early, gates)[0].get(hop, 0)
                sizes.setdefault(count, {}).setdefault((early, gates), []).append(k)
        for count, places in sizes.items():
            if count == 0:
                continue
            chosen = False
            for (early, gates), ks in places.items():
                when = (t < gate_steps) if gates else ((t >= gate_steps) & (t < split)) if early else (t >= split)
                if len(ks) < nz:
                    there = z == ks[0]
                    for k in ks[1:]:
                        there = there | (z == k)
                    when = when & there
                chosen = when if chosen is False else chosen | when

            @pl.when(chosen)
            def _():
                block = w_ref.at[0, pl.ds(0, count * shard)]
                pltpu.make_async_copy(block, block, hop_recv.at[t, hop]).wait()

    def own_first(t):
        @pl.when(z > 0)
        def _():
            along_z(t, z, z - 1, 1)

        @pl.when(z < last)
        def _():
            along_z(t, z, z + 1, 1)

        across(t, z, 0)

    def z_hop(t, distance):
        @pl.when((z >= distance) & (z < last))
        def _():
            along_z(t, z - distance, z + 1, distance + 1)

        @pl.when((z + distance < nz) & (z > 0))
        def _():
            along_z(t, z + distance, z - 1, distance + 1)

    def sideways(t, distance):
        @pl.when(z >= distance)
        def _():
            across(t, z - distance, last)

        @pl.when(z + distance < nz)
        def _():
            across(t, z + distance, last)

    def d_hop(t, distance):
        onward = (t >= split) | (distance + 1 < reach)

        @pl.when((z >= distance) & (z < last) & (onward | (z + 1 < last)))
        def _():
            diagonal(t, z - distance, z + 1, distance + 1)

        @pl.when((z + distance < nz) & (z > 0) & (onward | (z - 1 > 0)))
        def _():
            diagonal(t, z + distance, z - 1, distance + 1)

    far = last - z
    middle = jnp.where(z == 0, reach, 1)

    def hop_done(t, hop):
        wait_hop(t, hop)
        if hop + 1 < last:
            z_hop(t, hop + 1)
        if hop == 0:
            remote(unit(t, fx, z, 0, half), send, hop_recv.at[t, 1], (fy, z)).start()
            remote(unit(t, fy, z, half, half), send, hop_recv.at[t, 1], (fx, z)).start()
        if hop == 1:
            @pl.when(z > 0)
            def _():
                diagonal(t, z, z - 1, 1)

            @pl.when(z < last)
            def _():
                diagonal(t, z, z + 1, 1)
        if 2 <= hop < last:
            d_hop(t, hop - 1)
        if hop + 1 <= last:
            sideways(t, hop + 1)
        if hop + 1 == last:
            remote(whole_line(t, f), core, core_recv.at[t], (fc, z)).start()

            @pl.when(t < gate_steps)
            def _():
                for k in range(nz):
                    @pl.when(z != k)
                    def _():
                        remote(gate_of(t, k), gate_core_send.at[0], gate_core_recv.at[0], (fc, z)).start()
        if hop == last:
            @pl.when(at_end & (t < split))
            def _():
                remote(unit(t, fx, far), send, far_recv.at[t], (fy, z)).start()
                remote(unit(t, fy, middle), send, far_recv.at[t], (fx, z)).start()

            @pl.when(at_end & (t >= split))
            def _():
                remote(unit(t, fx, far, 0, half), send, far_recv.at[t], (fy, z)).start()
                remote(unit(t, fy, far, half, half), send, far_recv.at[t], (fx, z)).start()

            remote(whole_line(t, fx), core, core_recv.at[t], (fc, z)).start()
            remote(whole_line(t, fy), core, core_recv.at[t], (fc, z)).start()

    def corner_done(t):
        @pl.when(at_end & (t < split))
        def _():
            block = w_ref.at[0, pl.ds(0, 2 * shard)]
            pltpu.make_async_copy(block, block, far_recv.at[t]).wait()

        @pl.when(at_end & (t >= split))
        def _():
            block = w_ref.at[0, pl.ds(0, shard)]
            pltpu.make_async_copy(block, block, far_recv.at[t]).wait()

        remote(whole_line(t, fd), core, core_recv.at[t], (fc, z)).start()

    def multiply(t):
        whole = w_ref.at[t, pl.ds(0, 4 * line)]
        pltpu.make_async_copy(whole, whole, core_recv.at[t]).wait()
        column = columns(t % split)
        tall = TALL

        def body(i, _):
            at = pl.ds(pl.multiple_of(i * tall, tall), tall)
            product = jnp.dot(normed_ref[at, :], w_ref[t], preferred_element_type=jnp.float32)

            @pl.when(t < split)
            def _():
                rec_ref[at, column] = product.astype(jnp.bfloat16)

            @pl.when(t >= split)
            def _():
                h = jnp.maximum(t - split, 0)
                for j in range(pieces):
                    lanes = pl.ds(pl.multiple_of(h * channels + j * LANES, LANES), LANES)
                    state = b_ref[h * pieces + j, at, :] + a_ref[h * pieces + j, at, :] * start_ref[0:1, lanes]
                    act = jax.nn.gelu(product[:, j * LANES : (j + 1) * LANES], approximate=True)
                    out_ref[at, lanes] = (state * act).astype(out_ref.dtype)

            return 0

        lax.fori_loop(0, rows // tall, body, 0)

    def columns(h):
        return pl.ds(pl.multiple_of(h * channels, channels), channels)

    def tail_copy(h, source_rows, device):
        return pltpu.make_async_remote_copy(
            src_ref=rec_ref.at[pl.ds(source_rows, lead), columns(h)],
            dst_ref=before_ref.at[:, columns(h)],
            send_sem=tail_send.at[0], recv_sem=tail_recv.at[h],
            device_id=device, device_id_type=MESH,
        )

    def carry_copy(h, device):
        return pltpu.make_async_remote_copy(
            src_ref=carry_ref.at[:, columns(h)], dst_ref=start_ref.at[:, columns(h)],
            send_sem=carry_send.at[0], recv_sem=carry_recv.at[h],
            device_id=device, device_id_type=MESH,
        )

    def send_tail(h):
        @pl.when(z < last)
        def _():
            tail_copy(h, rows - lead, (f, z + 1)).start()

    def scan(h):
        @pl.when(z > 0)
        def _():
            tail_copy(h, rows - lead, (f, z)).wait_recv()

        cols = columns(h)
        padded_ref[pl.ds(0, lead), :] = before_ref[:, cols].astype(jnp.float32)
        padded_ref[pl.ds(lead, rows), :] = rec_ref[:, cols].astype(jnp.float32)
        conv_sum = jnp.zeros((rows, channels), jnp.float32) + bias_ref[:, cols]
        for tap in range(taps):
            conv_sum = conv_sum + weight_ref[tap : tap + 1, cols] * padded_ref[pl.ds(lead - tap, rows), :]
        conv_out = conv_sum.astype(jnp.bfloat16)
        gates = jnp.dot(conv_out, table_ref[cols, :], preferred_element_type=jnp.float32)
        input_gate = jax.nn.sigmoid(gates[:, :channels] + gate_bias_ref[0:1, cols])
        recur_gate = jax.nn.sigmoid(gates[:, channels:] + gate_bias_ref[1:2, cols])
        param = decay_ref[:, cols]
        softplus = jnp.maximum(param, 0.0) + jnp.log1p(jnp.exp(-jnp.abs(param)))
        log_decay = -8.0 * softplus * recur_gate
        decay = jnp.exp(log_decay)
        lost = -jnp.tanh(log_decay) * (decay * decay + 1.0)
        driven = jnp.sqrt(lost) * input_gate * conv_out.astype(jnp.float32)
        for j in range(pieces):
            a_ref[h * pieces + j] = decay[:, j * LANES : (j + 1) * LANES]
            b_ref[h * pieces + j] = driven[:, j * LANES : (j + 1) * LANES]

        lanes = 8
        length = rows // lanes

        def body(i, carry):
            at = pl.ds(i, lanes, stride=length)
            after = []
            for j in range(pieces):
                product, state = carry[j]
                decay_now = a_ref[h * pieces + j, at, :]
                product = product * decay_now
                state = decay_now * state + b_ref[h * pieces + j, at, :]
                a_ref[h * pieces + j, at, :] = product
                b_ref[h * pieces + j, at, :] = state
                after.append((product, state))
            return tuple(after)

        fresh = (jnp.ones((lanes, LANES), jnp.float32), jnp.zeros((lanes, LANES), jnp.float32))
        totals = lax.fori_loop(0, length, body, (fresh,) * pieces, unroll=8)
        for j in range(pieces):
            product, state = totals[j]
            start = jnp.zeros((1, LANES), jnp.float32)
            prefix = jnp.ones((1, LANES), jnp.float32)
            for i in range(lanes):
                at = pl.ds(i * length, length)
                within = a_ref[h * pieces + j, at, :]
                b_ref[h * pieces + j, at, :] = b_ref[h * pieces + j, at, :] + within * start
                a_ref[h * pieces + j, at, :] = within * prefix
                start = product[i : i + 1, :] * start + state[i : i + 1, :]
                prefix = prefix * product[i : i + 1, :]
            col = pl.ds(pl.multiple_of((h * pieces + j) * LANES, LANES), LANES)
            end_ref[0:1, col] = prefix
            end_ref[1:2, col] = start

    def make_carry(h):
        cols = columns(h)

        @pl.when(z > 0)
        def _():
            carry_copy(h, (f, z)).wait_recv()

        @pl.when(z < last)
        def _():
            end = end_ref[0:1, cols] * start_ref[0:1, cols] + end_ref[1:2, cols]
            carry_ref[:, cols] = jnp.broadcast_to(end, (carry_ref.shape[0], channels))

    def send_carry(h):
        @pl.when(z < last)
        def _():
            carry_copy(h, (f, z + 1)).start()

    @pl.when(z == 0)
    def _():
        before_ref[...] = jnp.zeros_like(before_ref)
        start_ref[...] = jnp.zeros_like(start_ref)

    hops = [(functools.partial(hop_done, hop=hop), LAGS[hop]) for hop in range(nz)]
    stages = hops[::-1] + [(corner_done, LAGS[nz]), (own_first, 0)]
    gates_at = LAGS[reach] + gate_steps
    finish = LAGS[nz] + 1
    tail_at = finish + 1
    scan_at = max(tail_at + 1, gates_at)
    steps = chunks + finish

    def on_head(s, first, stage):
        @pl.when((s >= first) & (s < first + heads))
        def _():
            stage(s - first)

    def step(s, _):
        for stage, lag in stages:
            @pl.when((s >= lag) & (s < chunks + lag))
            def _():
                stage(s - lag)

        on_head(s, scan_at + 2 + z, send_carry)
        on_head(s, tail_at, send_tail)

        @pl.when(s == gates_at)
        def _():
            others = table_ref.at[pl.ds(0, last * piece * gate_steps)]
            pltpu.make_async_copy(others, others, gate_core_recv.at[0]).wait()

        @pl.when(s == LAGS[0])
        def _():
            token_copy.wait()
            for copy in small:
                copy.wait()

        @pl.when((s >= LAGS[0]) & (s < LAGS[0] + NORM_PARTS))
        def _():
            normalise(normed_ref, gain_ref, s - LAGS[0], NORM_PARTS)

        @pl.when((s >= finish) & (s < chunks + finish))
        def _():
            multiply(s - finish)

        on_head(s, scan_at, scan)
        on_head(s, scan_at + 1 + z, make_carry)
        return 0

    lax.fori_loop(0, steps, step, 0)

    for k in range(nz):
        early, late = hop_counts(nz, k, True, False), hop_counts(nz, k, False, False)

        @pl.when(z == k)
        def _():
            total = split * (early[2] + late[2])
            deep = max(n for n in range(1, chunks + 1) if total % n == 0)
            sent = w_ref.at[pl.ds(0, deep), pl.ds(0, total // deep * shard)]
            pltpu.make_async_copy(sent, sent, send).wait()
            sent_gate = table_ref.at[pl.ds(0, early[3] * piece * gate_steps)]
            pltpu.make_async_copy(sent_gate, sent_gate, gate_send.at[0]).wait()

    whole = w_ref.at[:, pl.ds(0, 4 * line)]
    pltpu.make_async_copy(whole, whole, core).wait()
    others = table_ref.at[pl.ds(0, last * piece * gate_steps)]
    pltpu.make_async_copy(others, others, gate_core_send.at[0]).wait()

    @pl.when(z < last)
    def _():
        pltpu.make_async_copy(before_ref, before_ref, tail_send.at[0]).wait()
        pltpu.make_async_copy(carry_ref, carry_ref, carry_send.at[0]).wait()


def fused_branch(
    nz, tokens, norm_gain, lru_proj, gelu_proj, conv_weight, conv_bias, gate_weights, gate_bias,
    decay_param,
):
    rows, width = tokens.shape
    inner = lru_proj.shape[1]
    channels = gate_weights.shape[1] // 2
    chunks = 2 * inner // channels
    heads = inner // channels
    any_ = pl.BlockSpec(memory_space=pl.ANY)
    dma = pltpu.SemaphoreType.DMA
    f32, bf16 = jnp.float32, jnp.bfloat16
    lead = 16
    return pl.pallas_call(
        functools.partial(branch_kernel, nz),
        out_shape=pltpu.VMEM((rows, inner), bf16),
        in_specs=[any_] * 9,
        out_specs=pl.BlockSpec(memory_space=pltpu.VMEM),
        scratch_shapes=[
            pltpu.VMEM((1, width), f32), pltpu.VMEM(conv_weight.shape, f32), pltpu.VMEM((1, inner), f32),
            pltpu.VMEM(gate_bias.shape, f32), pltpu.VMEM((1, inner), f32),
            pltpu.VMEM((chunks, width, channels), bf16),
            pltpu.VMEM((rows, width), bf16),
            pltpu.VMEM((rows, inner), bf16),
            pltpu.VMEM((gate_weights.shape[0] * nz, 2 * channels), bf16),
            pltpu.VMEM((lead, inner), bf16),
            pltpu.VMEM((lead + rows, channels), f32),
            pltpu.VMEM((inner // LANES, rows, LANES), f32),
            pltpu.VMEM((inner // LANES, rows, LANES), f32),
            pltpu.VMEM((8, inner), f32), pltpu.VMEM((8, inner), f32), pltpu.VMEM((8, inner), f32),
            dma((8,)), dma((1,)), dma((1,)), dma((1,)), dma((1,)), dma((1,)), dma((1,)), dma((1,)),
            dma((chunks, nz)), dma((chunks,)), dma((chunks,)), dma((1,)),
            dma((heads,)), dma((heads,)),
        ],
        compiler_params=pltpu.CompilerParams(
            collective_id=0, has_side_effects=True, vmem_limit_bytes=VMEM_BYTES
        ),
    )(
        tokens, norm_gain.reshape(1, width), lru_proj, gelu_proj, gate_weights, conv_weight,
        conv_bias.reshape(1, inner), gate_bias, decay_param.reshape(1, inner),
    )


def scan_kernel(
    rec_ref, before_ref, weight_ref, bias_ref, table_ref, gate_bias_ref, decay_ref,
    state_ref, cumulative_ref, end_ref, padded_ref, a_ref, b_ref,
):
    rows, channels = rec_ref.shape
    taps = weight_ref.shape[0]
    lead = before_ref.shape[0]
    padded_ref[pl.ds(0, lead), :] = before_ref[...].astype(jnp.float32)
    padded_ref[pl.ds(lead, rows), :] = rec_ref[...].astype(jnp.float32)
    conv_sum = jnp.zeros((rows, channels), jnp.float32) + bias_ref[...]
    for tap in range(taps):
        conv_sum = conv_sum + weight_ref[tap : tap + 1, :] * padded_ref[pl.ds(lead - tap, rows), :]
    conv_out = conv_sum.astype(jnp.bfloat16)
    gates = jnp.dot(conv_out, table_ref[...], preferred_element_type=jnp.float32)
    input_gate = jax.nn.sigmoid(gates[:, :channels] + gate_bias_ref[0:1, :])
    recur_gate = jax.nn.sigmoid(gates[:, channels:] + gate_bias_ref[1:2, :])
    param = decay_ref[...]
    softplus = jnp.maximum(param, 0.0) + jnp.log1p(jnp.exp(-jnp.abs(param)))
    log_decay = -8.0 * softplus * recur_gate
    decay = jnp.exp(log_decay)
    lost = -jnp.tanh(log_decay) * (decay * decay + 1.0)
    driven = jnp.sqrt(lost) * input_gate * conv_out.astype(jnp.float32)
    parts = channels // LANES
    for j in range(parts):
        a_ref[j] = decay[:, j * LANES : (j + 1) * LANES]
        b_ref[j] = driven[:, j * LANES : (j + 1) * LANES]

    lanes = 8
    length = rows // lanes

    def body(i, carry):
        at = pl.ds(i, lanes, stride=length)
        after = []
        for j in range(parts):
            product, state = carry[j]
            decay_now = a_ref[j, at, :]
            product = product * decay_now
            state = decay_now * state + b_ref[j, at, :]
            a_ref[j, at, :] = product
            b_ref[j, at, :] = state
            after.append((product, state))
        return tuple(after)

    fresh = (jnp.ones((lanes, LANES), jnp.float32), jnp.zeros((lanes, LANES), jnp.float32))
    totals = lax.fori_loop(0, length, body, (fresh,) * parts, unroll=8)
    for j in range(parts):
        product, state = totals[j]
        cols = slice(j * LANES, (j + 1) * LANES)
        start = jnp.zeros((1, LANES), jnp.float32)
        prefix = jnp.ones((1, LANES), jnp.float32)
        for i in range(lanes):
            at = pl.ds(i * length, length)
            within = a_ref[j, at, :]
            state_ref[at, cols] = b_ref[j, at, :] + within * start
            cumulative_ref[at, cols] = within * prefix
            start = product[i : i + 1, :] * start + state[i : i + 1, :]
            prefix = prefix * product[i : i + 1, :]
        end_ref[0:1, cols] = prefix
        end_ref[1:2, cols] = start


def local_scan(rec, before, conv_weight, conv_bias, table, gate_bias, decay_param):
    rows, inner = rec.shape
    width = table.shape[1] // 2
    lead = before.shape[0]

    def columns(height):
        return pl.BlockSpec((height, width), lambda h: (0, h))

    return pl.pallas_call(
        scan_kernel,
        grid=(inner // width,),
        out_shape=(
            jax.ShapeDtypeStruct((rows, inner), jnp.float32),
            jax.ShapeDtypeStruct((rows, inner), jnp.float32),
            jax.ShapeDtypeStruct((2, inner), jnp.float32),
        ),
        in_specs=[
            columns(rows), columns(lead), columns(conv_weight.shape[0]), columns(1),
            pl.BlockSpec((width, 2 * width), lambda h: (h, 0)), columns(2), columns(1),
        ],
        out_specs=(columns(rows), columns(rows), columns(2)),
        scratch_shapes=[
            pltpu.VMEM((rows + lead, width), jnp.float32),
            pltpu.VMEM((width // LANES, rows, LANES), jnp.float32),
            pltpu.VMEM((width // LANES, rows, LANES), jnp.float32),
        ],
    )(
        rec, before, conv_weight, conv_bias.reshape(1, inner), table, gate_bias,
        decay_param.reshape(1, inner),
    )


def shards(
    nz, paired, tokens, norm_gain, lru_proj, gelu_proj, conv_weight, conv_bias, gate_weights,
    gate_bias, decay_param,
):
    seq_count, tok_rows, width = tokens.shape
    inner = lru_proj.shape[1]
    taps = conv_weight.shape[0]
    if paired:
        out = fused_branch(
            nz, tokens.reshape(tok_rows, width), norm_gain, lru_proj, gelu_proj, conv_weight,
            conv_bias, gate_weights, gate_bias, decay_param,
        )
        return out.reshape(seq_count, tok_rows, inner)
    flat = tokens.reshape(tok_rows, width).astype(jnp.float32)
    mean_square = jnp.mean(flat * flat, axis=-1, keepdims=True)
    normed = (flat * lax.rsqrt(mean_square + 1e-06) * norm_gain).astype(jnp.bfloat16)
    every = [
        lax.all_gather(w, ("fsdp", "seq"), axis=0, tiled=True) for w in (lru_proj, gelu_proj)
    ]
    rec = jnp.dot(normed, every[0], preferred_element_type=jnp.float32).astype(jnp.bfloat16)
    act = jnp.dot(normed, every[1], preferred_element_type=jnp.float32)
    table = lax.all_gather(gate_weights, "seq", axis=0, tiled=True)
    lead = 8
    before = lax.ppermute(
        rec[tok_rows - lead :, :], "seq", [(i, i + 1) for i in range(nz - 1)]
    )
    local, cumulative, ends = local_scan(
        rec, before, conv_weight, conv_bias, table, gate_bias, decay_param
    )
    every_end = lax.all_gather(ends, "seq")
    position = lax.axis_index("seq")
    start = jnp.zeros((inner,), jnp.float32)
    for k in range(nz - 1):
        start = jnp.where(k < position, every_end[k, 0] * start + every_end[k, 1], start)
    gelu = jax.nn.gelu(act, approximate=True)
    out = ((local + cumulative * start) * gelu).astype(jnp.bfloat16)
    return out.reshape(seq_count, tok_rows, inner)


def solution(mesh):
    placed = (
        P("fsdp", "seq", None), P(), P(("fsdp", "seq"), None), P(("fsdp", "seq"), None), P(), P(),
        P("seq", None), P(), P(),
    )
    nz = mesh.shape["seq"]
    paired = mesh.shape["fsdp"] == 8 and nz == len(LAGS) - 1
    return jax.shard_map(
        functools.partial(shards, nz, paired), mesh=mesh, in_specs=placed,
        out_specs=P("fsdp", "seq", None), check_vma=False,
    )
```

```python
import functools

import jax
import jax.numpy as jnp
from jax import lax
from jax.experimental import pallas as pl
from jax.experimental.pallas import tpu as pltpu
from jax.sharding import PartitionSpec as P

MESH = pl.DeviceIdType.MESH
LANES = 128
VMEM_BYTES = 58_000_000


def normalise(normed_ref, gain_ref, part, parts):
    rows = 32

    def body(i, _):
        at = pl.ds(pl.multiple_of(i * rows, rows), rows)
        values = normed_ref[at, :].astype(jnp.float32)
        mean_square = jnp.mean(values * values, axis=-1, keepdims=True)
        normed_ref[at, :] = (values * lax.rsqrt(mean_square + 1e-06) * gain_ref[...]).astype(jnp.bfloat16)
        return 0

    blocks = normed_ref.shape[0] // rows // parts
    lax.fori_loop(part * blocks, (part + 1) * blocks, body, 0)


LAGS = (5, 9, 12, 14, 15)
NORM_PARTS = 4
TALL = 512
EXTRA = 1
SLACK = 0


def hop_counts(nz, k, early, gates):
    last, reach = nz - 1, nz - 2
    twice = 2 if gates else 1
    end = k in (0, last)
    got = {0: 2, 1: 1}
    for distance in range(1, nz):
        sources = int(k >= distance) + int(k + distance < nz)
        got[distance - 1] = got.get(distance - 1, 0) + twice * sources
        if distance <= reach:
            for source in (k - distance, k + distance):
                if 0 <= source < nz and not (early and end and distance == reach):
                    got[distance + 1] = got.get(distance + 1, 0) + 1
    got[last] = got.get(last, 0) + 2 * last
    far = (2 if early else 1) if end else 0
    sent = 2 + 2 * last + 1 + far
    for source in range(nz):
        for target in (k - 1, k + 1):
            onward = (target - k) * (k - source) >= 0
            if not (0 <= target < nz and onward):
                continue
            sent += 1
            distance = abs(target - source)
            closed = early and target in (0, last) and distance == reach
            if distance <= reach and not closed:
                sent += 1
    passed = sum(
        1 for source in range(nz) for target in (k - 1, k + 1)
        if 0 <= target < nz and (target - k) * (k - source) >= 0
    )
    return got, far, sent, passed


def branch_kernel(
    nz,
    tokens_ref, gain_in, lru_ref, gelu_ref, gate_ref,
    weight_in, bias_in, gate_bias_in, decay_in,
    out_ref,
    gain_ref, weight_ref, bias_ref, gate_bias_ref, decay_ref,
    w_ref, normed_ref, rec_ref, table_ref, before_ref, padded_ref, a_ref, b_ref,
    end_ref, carry_ref, start_ref,
    own_sem, out_sem, send_sem, core_send, gate_send, gate_core_send, tail_send, carry_send,
    hop_recv, far_recv, core_recv, gate_core_recv, tail_recv, carry_recv,
):
    f = lax.axis_index("fsdp")
    z = lax.axis_index("seq")
    c, x, y = f % 2, (f // 2) % 2, f // 4
    fx, fy, fc = f + 2 - 4 * x, f + 4 - 8 * y, f + 1 - 2 * c
    fd = fx + 4 - 8 * y
    shard = lru_ref.shape[0]
    line = shard * nz
    half = shard // 2
    chunks, _, wide = w_ref.shape
    split = chunks // 2
    early_chunks = split + EXTRA
    gate_rows = gate_ref.shape[0]
    gate_steps = split // 2
    piece = gate_rows // 2 // gate_steps
    rows = normed_ref.shape[0]
    channels = table_ref.shape[1] // 2
    heads = rec_ref.shape[1] // channels
    pieces = channels // LANES
    taps = weight_ref.shape[0]
    lead = before_ref.shape[0]
    last = nz - 1
    reach = nz - 2
    at_end = (z == 0) | (z == last)

    def remote(src, send, recv, device):
        return pltpu.make_async_remote_copy(
            src_ref=src, dst_ref=src, send_sem=send, recv_sem=recv,
            device_id=device, device_id_type=MESH,
        )

    own = pl.ds(pl.multiple_of((f * nz + z) * shard, shard), shard)
    for t in range(chunks):
        src = lru_ref if t < split else gelu_ref
        cols = pl.ds((t % split) * wide, wide)
        pltpu.make_async_copy(src.at[:, cols], w_ref.at[t, own], own_sem.at[0]).start()
    own_gate = pl.ds(pl.multiple_of(z * gate_rows, gate_rows), gate_rows)
    gate_copy = pltpu.make_async_copy(gate_ref, table_ref.at[own_gate], own_sem.at[1])
    gate_copy.start()
    token_copy = pltpu.make_async_copy(tokens_ref, normed_ref, own_sem.at[2])
    token_copy.start()
    small = [
        pltpu.make_async_copy(source, target, own_sem.at[3 + i])
        for i, (source, target) in enumerate((
            (gain_in, gain_ref), (weight_in, weight_ref), (bias_in, bias_ref),
            (gate_bias_in, gate_bias_ref), (decay_in, decay_ref),
        ))
    ]
    for copy in small:
        copy.start()

    barrier = pltpu.get_barrier_semaphore()
    for device in ((fx, z), (fy, z), (fc, z)):
        pl.semaphore_signal(barrier, inc=1, device_id=device, device_id_type=MESH)

    @pl.when(z > 0)
    def _():
        pl.semaphore_signal(barrier, inc=1, device_id=(f, z - 1), device_id_type=MESH)

    @pl.when(z < last)
    def _():
        pl.semaphore_signal(barrier, inc=1, device_id=(f, z + 1), device_id_type=MESH)

    for k in range(nz):
        @pl.when(z == k)
        def _():
            pl.semaphore_wait(barrier, 3 + int(k > 0) + int(k < last))

    pltpu.make_async_copy(w_ref.at[:, own], w_ref.at[:, own], own_sem.at[0]).wait()
    gate_copy.wait()

    def unit(t, owner, k, first=0, size=shard):
        start = (owner * nz + k) * shard + first
        return w_ref.at[t, pl.ds(pl.multiple_of(start, half), size)]

    def whole_line(t, owner):
        return w_ref.at[t, pl.ds(pl.multiple_of(owner * line, line), line)]

    def gate_of(t, source):
        first = source * gate_rows + c * (gate_rows // 2) + t * piece
        return table_ref.at[pl.ds(pl.multiple_of(first, piece), piece)]

    core = core_send.at[0]

    def sender(t):
        return send_sem.at[jnp.where(t < early_chunks, 0, 1)]

    def along_z(t, k, target, distance):
        remote(unit(t, f, k), sender(t), hop_recv.at[t, distance - 1], (f, target)).start()

        @pl.when(t < gate_steps)
        def _():
            remote(gate_of(t, k), gate_send.at[0], hop_recv.at[t, distance - 1], (f, target)).start()

    def across(t, k, hop):
        remote(unit(t, f, k), sender(t), hop_recv.at[t, hop], (fx, z)).start()
        remote(unit(t, f, k), sender(t), hop_recv.at[t, hop], (fy, z)).start()

    def diagonal(t, k, target, distance):
        remote(unit(t, fd, k), sender(t), hop_recv.at[t, distance + 1], (f, target)).start()

    def wait_hop(t, hop):
        sizes = {}
        for k in range(nz):
            for early, gates in ((True, True), (True, False), (False, False)):
                count = hop_counts(nz, k, early, gates)[0].get(hop, 0)
                sizes.setdefault(count, {}).setdefault((early, gates), []).append(k)
        for count, places in sizes.items():
            if count == 0:
                continue
            chosen = False
            for (early, gates), ks in places.items():
                when = (t < gate_steps) if gates else ((t >= gate_steps) & (t < early_chunks)) if early else (t >= early_chunks)
                if len(ks) < nz:
                    there = z == ks[0]
                    for k in ks[1:]:
                        there = there | (z == k)
                    when = when & there
                chosen = when if chosen is False else chosen | when

            @pl.when(chosen)
            def _():
                block = w_ref.at[0, pl.ds(0, count * shard)]
                pltpu.make_async_copy(block, block, hop_recv.at[t, hop]).wait()

    def own_first(t):
        @pl.when(z > 0)
        def _():
            along_z(t, z, z - 1, 1)

        @pl.when(z < last)
        def _():
            along_z(t, z, z + 1, 1)

        across(t, z, 0)

    def z_hop(t, distance):
        @pl.when((z >= distance) & (z < last))
        def _():
            along_z(t, z - distance, z + 1, distance + 1)

        @pl.when((z + distance < nz) & (z > 0))
        def _():
            along_z(t, z + distance, z - 1, distance + 1)

    def sideways(t, distance):
        @pl.when(z >= distance)
        def _():
            across(t, z - distance, last)

        @pl.when(z + distance < nz)
        def _():
            across(t, z + distance, last)

    def d_hop(t, distance):
        onward = (t >= early_chunks) | (distance + 1 < reach)

        @pl.when((z >= distance) & (z < last) & (onward | (z + 1 < last)))
        def _():
            diagonal(t, z - distance, z + 1, distance + 1)

        @pl.when((z + distance < nz) & (z > 0) & (onward | (z - 1 > 0)))
        def _():
            diagonal(t, z + distance, z - 1, distance + 1)

    far = last - z
    middle = jnp.where(z == 0, reach, 1)

    def hop_done(t, hop):
        wait_hop(t, hop)
        if hop + 1 < last:
            z_hop(t, hop + 1)
        if hop == 0:
            remote(unit(t, fx, z, 0, half), sender(t), hop_recv.at[t, 1], (fy, z)).start()
            remote(unit(t, fy, z, half, half), sender(t), hop_recv.at[t, 1], (fx, z)).start()
        if hop == 1:
            @pl.when(z > 0)
            def _():
                diagonal(t, z, z - 1, 1)

            @pl.when(z < last)
            def _():
                diagonal(t, z, z + 1, 1)
        if 2 <= hop < last:
            d_hop(t, hop - 1)
        if hop + 1 <= last:
            sideways(t, hop + 1)
        if hop + 1 == last:
            remote(whole_line(t, f), core, core_recv.at[t], (fc, z)).start()

            @pl.when(t < gate_steps)
            def _():
                for k in range(nz):
                    @pl.when(z != k)
                    def _():
                        remote(gate_of(t, k), gate_core_send.at[0], gate_core_recv.at[0], (fc, z)).start()
        if hop == last:
            @pl.when(at_end & (t < early_chunks))
            def _():
                remote(unit(t, fx, far), sender(t), far_recv.at[t], (fy, z)).start()
                remote(unit(t, fy, middle), sender(t), far_recv.at[t], (fx, z)).start()

            @pl.when(at_end & (t >= early_chunks))
            def _():
                remote(unit(t, fx, far, 0, half), sender(t), far_recv.at[t], (fy, z)).start()
                remote(unit(t, fy, far, half, half), sender(t), far_recv.at[t], (fx, z)).start()

            remote(whole_line(t, fx), core, core_recv.at[t], (fc, z)).start()
            remote(whole_line(t, fy), core, core_recv.at[t], (fc, z)).start()

    def corner_done(t):
        @pl.when(at_end & (t < early_chunks))
        def _():
            block = w_ref.at[0, pl.ds(0, 2 * shard)]
            pltpu.make_async_copy(block, block, far_recv.at[t]).wait()

        @pl.when(at_end & (t >= early_chunks))
        def _():
            block = w_ref.at[0, pl.ds(0, shard)]
            pltpu.make_async_copy(block, block, far_recv.at[t]).wait()

        remote(whole_line(t, fd), core, core_recv.at[t], (fc, z)).start()

    def multiply(t):
        whole = w_ref.at[t, pl.ds(0, 4 * line)]
        pltpu.make_async_copy(whole, whole, core_recv.at[t]).wait()
        column = columns(t % split)
        tall = TALL

        def body(i, _):
            at = pl.ds(pl.multiple_of(i * tall, tall), tall)
            product = jnp.dot(normed_ref[at, :], w_ref[t], preferred_element_type=jnp.float32)

            @pl.when(t < split)
            def _():
                rec_ref[at, column] = product.astype(jnp.bfloat16)

            @pl.when(t >= split)
            def _():
                h = jnp.maximum(t - split, 0)
                for j in range(pieces):
                    lanes = pl.ds(pl.multiple_of(h * channels + j * LANES, LANES), LANES)
                    state = b_ref[h * pieces + j, at, :] + a_ref[h * pieces + j, at, :] * start_ref[h, :, j * LANES : (j + 1) * LANES]
                    act = jax.nn.gelu(product[:, j * LANES : (j + 1) * LANES], approximate=True)
                    out_ref[at, lanes] = (state * act).astype(out_ref.dtype)

            return 0

        lax.fori_loop(0, rows // tall, body, 0)

    def columns(h):
        return pl.ds(pl.multiple_of(h * channels, channels), channels)

    def tail_copy(h, source_rows, device):
        return pltpu.make_async_remote_copy(
            src_ref=rec_ref.at[pl.ds(source_rows, lead), columns(h)],
            dst_ref=before_ref.at[:, columns(h)],
            send_sem=tail_send.at[0], recv_sem=tail_recv.at[h],
            device_id=device, device_id_type=MESH,
        )

    def carry_copy(h, device):
        return pltpu.make_async_remote_copy(
            src_ref=carry_ref.at[h], dst_ref=start_ref.at[h],
            send_sem=carry_send.at[0], recv_sem=carry_recv.at[h],
            device_id=device, device_id_type=MESH,
        )

    def send_tail(h):
        @pl.when(z < last)
        def _():
            tail_copy(h, rows - lead, (f, z + 1)).start()

    def scan(h):
        @pl.when(z > 0)
        def _():
            tail_copy(h, rows - lead, (f, z)).wait_recv()

        cols = columns(h)
        padded_ref[pl.ds(0, lead), :] = before_ref[:, cols].astype(jnp.float32)
        padded_ref[pl.ds(lead, rows), :] = rec_ref[:, cols].astype(jnp.float32)
        conv_sum = jnp.zeros((rows, channels), jnp.float32) + bias_ref[:, cols]
        for tap in range(taps):
            conv_sum = conv_sum + weight_ref[tap : tap + 1, cols] * padded_ref[pl.ds(lead - tap, rows), :]
        conv_out = conv_sum.astype(jnp.bfloat16)
        gates = jnp.dot(conv_out, table_ref[cols, :], preferred_element_type=jnp.float32)
        input_gate = jax.nn.sigmoid(gates[:, :channels] + gate_bias_ref[0:1, cols])
        recur_gate = jax.nn.sigmoid(gates[:, channels:] + gate_bias_ref[1:2, cols])
        param = decay_ref[:, cols]
        softplus = jnp.maximum(param, 0.0) + jnp.log1p(jnp.exp(-jnp.abs(param)))
        log_decay = -8.0 * softplus * recur_gate
        decay = jnp.exp(log_decay)
        lost = -jnp.tanh(log_decay) * (decay * decay + 1.0)
        driven = jnp.sqrt(lost) * input_gate * conv_out.astype(jnp.float32)
        for j in range(pieces):
            a_ref[h * pieces + j] = decay[:, j * LANES : (j + 1) * LANES]
            b_ref[h * pieces + j] = driven[:, j * LANES : (j + 1) * LANES]

        lanes = 8
        length = rows // lanes

        def body(i, carry):
            at = pl.ds(i, lanes, stride=length)
            after = []
            for j in range(pieces):
                product, state = carry[j]
                decay_now = a_ref[h * pieces + j, at, :]
                product = product * decay_now
                state = decay_now * state + b_ref[h * pieces + j, at, :]
                a_ref[h * pieces + j, at, :] = product
                b_ref[h * pieces + j, at, :] = state
                after.append((product, state))
            return tuple(after)

        fresh = (jnp.ones((lanes, LANES), jnp.float32), jnp.zeros((lanes, LANES), jnp.float32))
        totals = lax.fori_loop(0, length, body, (fresh,) * pieces, unroll=8)
        for j in range(pieces):
            product, state = totals[j]
            start = jnp.zeros((1, LANES), jnp.float32)
            prefix = jnp.ones((1, LANES), jnp.float32)
            for i in range(lanes):
                at = pl.ds(i * length, length)
                within = a_ref[h * pieces + j, at, :]
                b_ref[h * pieces + j, at, :] = b_ref[h * pieces + j, at, :] + within * start
                a_ref[h * pieces + j, at, :] = within * prefix
                start = product[i : i + 1, :] * start + state[i : i + 1, :]
                prefix = prefix * product[i : i + 1, :]
            col = pl.ds(pl.multiple_of((h * pieces + j) * LANES, LANES), LANES)
            end_ref[0:1, col] = prefix
            end_ref[1:2, col] = start

    def make_carry(h):
        cols = columns(h)

        @pl.when(z > 0)
        def _():
            carry_copy(h, (f, z)).wait_recv()

        @pl.when(z < last)
        def _():
            carry_ref[h] = end_ref[0:1, cols] * start_ref[h] + end_ref[1:2, cols]

    def send_carry(h):
        @pl.when(z < last)
        def _():
            carry_copy(h, (f, z + 1)).start()

    @pl.when(z == 0)
    def _():
        before_ref[...] = jnp.zeros_like(before_ref)
        start_ref[...] = jnp.zeros_like(start_ref)

    hops = [(functools.partial(hop_done, hop=hop), LAGS[hop]) for hop in range(nz)]
    stages = hops[::-1] + [(corner_done, LAGS[nz]), (own_first, 0)]
    gates_at = LAGS[reach] + gate_steps
    finish = LAGS[nz] + 1
    tail_at = finish + 1
    scan_at = max(tail_at + 1 + SLACK, gates_at)
    steps = chunks + finish

    def on_head(s, first, stage):
        @pl.when((s >= first) & (s < first + heads))
        def _():
            stage(s - first)

    def step(s, _):
        on_head(s, scan_at + 2 + z, send_carry)
        on_head(s, tail_at, send_tail)

        for stage, lag in stages:
            @pl.when((s >= lag) & (s < chunks + lag))
            def _():
                stage(s - lag)

        @pl.when(s == gates_at)
        def _():
            others = table_ref.at[pl.ds(0, last * piece * gate_steps)]
            pltpu.make_async_copy(others, others, gate_core_recv.at[0]).wait()

        @pl.when(s == LAGS[0])
        def _():
            token_copy.wait()
            for copy in small:
                copy.wait()

        @pl.when((s >= LAGS[0]) & (s < LAGS[0] + NORM_PARTS))
        def _():
            normalise(normed_ref, gain_ref, s - LAGS[0], NORM_PARTS)

        @pl.when((s >= finish) & (s < chunks + finish))
        def _():
            multiply(s - finish)

        on_head(s, scan_at, scan)
        on_head(s, scan_at + 1 + z, make_carry)
        return 0

    lax.fori_loop(0, steps, step, 0)

    for k in range(nz):
        early, late = hop_counts(nz, k, True, False), hop_counts(nz, k, False, False)

        @pl.when(z == k)
        def _():
            for i, (depth, counts) in enumerate(((early_chunks, early), (chunks - early_chunks, late))):
                sent = w_ref.at[pl.ds(0, depth), pl.ds(0, counts[2] * shard)]
                pltpu.make_async_copy(sent, sent, send_sem.at[i]).wait()
            sent_gate = table_ref.at[pl.ds(0, early[3] * piece * gate_steps)]
            pltpu.make_async_copy(sent_gate, sent_gate, gate_send.at[0]).wait()

    whole = w_ref.at[:, pl.ds(0, 4 * line)]
    pltpu.make_async_copy(whole, whole, core).wait()
    others = table_ref.at[pl.ds(0, last * piece * gate_steps)]
    pltpu.make_async_copy(others, others, gate_core_send.at[0]).wait()

    @pl.when(z < last)
    def _():
        pltpu.make_async_copy(before_ref, before_ref, tail_send.at[0]).wait()
        pltpu.make_async_copy(carry_ref, carry_ref, carry_send.at[0]).wait()


def fused_branch(
    nz, tokens, norm_gain, lru_proj, gelu_proj, conv_weight, conv_bias, gate_weights, gate_bias,
    decay_param,
):
    rows, width = tokens.shape
    inner = lru_proj.shape[1]
    channels = gate_weights.shape[1] // 2
    chunks = 2 * inner // channels
    heads = inner // channels
    any_ = pl.BlockSpec(memory_space=pl.ANY)
    dma = pltpu.SemaphoreType.DMA
    f32, bf16 = jnp.float32, jnp.bfloat16
    lead = 8
    return pl.pallas_call(
        functools.partial(branch_kernel, nz),
        out_shape=pltpu.VMEM((rows, inner), bf16),
        in_specs=[any_] * 9,
        out_specs=pl.BlockSpec(memory_space=pltpu.VMEM),
        scratch_shapes=[
            pltpu.VMEM((1, width), f32), pltpu.VMEM(conv_weight.shape, f32), pltpu.VMEM((1, inner), f32),
            pltpu.VMEM(gate_bias.shape, f32), pltpu.VMEM((1, inner), f32),
            pltpu.VMEM((chunks, width, channels), bf16),
            pltpu.VMEM((rows, width), bf16),
            pltpu.VMEM((rows, inner), bf16),
            pltpu.VMEM((gate_weights.shape[0] * nz, 2 * channels), bf16),
            pltpu.VMEM((lead, inner), bf16),
            pltpu.VMEM((lead + rows, channels), f32),
            pltpu.VMEM((inner // LANES, rows, LANES), f32),
            pltpu.VMEM((inner // LANES, rows, LANES), f32),
            pltpu.VMEM((8, inner), f32), pltpu.VMEM((heads, 1, channels), f32), pltpu.VMEM((heads, 1, channels), f32),
            dma((8,)), dma((1,)), dma((2,)), dma((1,)), dma((1,)), dma((1,)), dma((1,)), dma((1,)),
            dma((chunks, nz)), dma((chunks,)), dma((chunks,)), dma((1,)),
            dma((heads,)), dma((heads,)),
        ],
        compiler_params=pltpu.CompilerParams(
            collective_id=0, has_side_effects=True, vmem_limit_bytes=VMEM_BYTES
        ),
    )(
        tokens, norm_gain.reshape(1, width), lru_proj, gelu_proj, gate_weights, conv_weight,
        conv_bias.reshape(1, inner), gate_bias, decay_param.reshape(1, inner),
    )


def scan_kernel(
    rec_ref, before_ref, weight_ref, bias_ref, table_ref, gate_bias_ref, decay_ref,
    state_ref, cumulative_ref, end_ref, padded_ref, a_ref, b_ref,
):
    rows, channels = rec_ref.shape
    taps = weight_ref.shape[0]
    lead = before_ref.shape[0]
    padded_ref[pl.ds(0, lead), :] = before_ref[...].astype(jnp.float32)
    padded_ref[pl.ds(lead, rows), :] = rec_ref[...].astype(jnp.float32)
    conv_sum = jnp.zeros((rows, channels), jnp.float32) + bias_ref[...]
    for tap in range(taps):
        conv_sum = conv_sum + weight_ref[tap : tap + 1, :] * padded_ref[pl.ds(lead - tap, rows), :]
    conv_out = conv_sum.astype(jnp.bfloat16)
    gates = jnp.dot(conv_out, table_ref[...], preferred_element_type=jnp.float32)
    input_gate = jax.nn.sigmoid(gates[:, :channels] + gate_bias_ref[0:1, :])
    recur_gate = jax.nn.sigmoid(gates[:, channels:] + gate_bias_ref[1:2, :])
    param = decay_ref[...]
    softplus = jnp.maximum(param, 0.0) + jnp.log1p(jnp.exp(-jnp.abs(param)))
    log_decay = -8.0 * softplus * recur_gate
    decay = jnp.exp(log_decay)
    lost = -jnp.tanh(log_decay) * (decay * decay + 1.0)
    driven = jnp.sqrt(lost) * input_gate * conv_out.astype(jnp.float32)
    parts = channels // LANES
    for j in range(parts):
        a_ref[j] = decay[:, j * LANES : (j + 1) * LANES]
        b_ref[j] = driven[:, j * LANES : (j + 1) * LANES]

    lanes = 8
    length = rows // lanes

    def body(i, carry):
        at = pl.ds(i, lanes, stride=length)
        after = []
        for j in range(parts):
            product, state = carry[j]
            decay_now = a_ref[j, at, :]
            product = product * decay_now
            state = decay_now * state + b_ref[j, at, :]
            a_ref[j, at, :] = product
            b_ref[j, at, :] = state
            after.append((product, state))
        return tuple(after)

    fresh = (jnp.ones((lanes, LANES), jnp.float32), jnp.zeros((lanes, LANES), jnp.float32))
    totals = lax.fori_loop(0, length, body, (fresh,) * parts, unroll=8)
    for j in range(parts):
        product, state = totals[j]
        cols = slice(j * LANES, (j + 1) * LANES)
        start = jnp.zeros((1, LANES), jnp.float32)
        prefix = jnp.ones((1, LANES), jnp.float32)
        for i in range(lanes):
            at = pl.ds(i * length, length)
            within = a_ref[j, at, :]
            state_ref[at, cols] = b_ref[j, at, :] + within * start
            cumulative_ref[at, cols] = within * prefix
            start = product[i : i + 1, :] * start + state[i : i + 1, :]
            prefix = prefix * product[i : i + 1, :]
        end_ref[0:1, cols] = prefix
        end_ref[1:2, cols] = start


def local_scan(rec, before, conv_weight, conv_bias, table, gate_bias, decay_param):
    rows, inner = rec.shape
    width = table.shape[1] // 2
    lead = before.shape[0]

    def columns(height):
        return pl.BlockSpec((height, width), lambda h: (0, h))

    return pl.pallas_call(
        scan_kernel,
        grid=(inner // width,),
        out_shape=(
            jax.ShapeDtypeStruct((rows, inner), jnp.float32),
            jax.ShapeDtypeStruct((rows, inner), jnp.float32),
            jax.ShapeDtypeStruct((2, inner), jnp.float32),
        ),
        in_specs=[
            columns(rows), columns(lead), columns(conv_weight.shape[0]), columns(1),
            pl.BlockSpec((width, 2 * width), lambda h: (h, 0)), columns(2), columns(1),
        ],
        out_specs=(columns(rows), columns(rows), columns(2)),
        scratch_shapes=[
            pltpu.VMEM((rows + lead, width), jnp.float32),
            pltpu.VMEM((width // LANES, rows, LANES), jnp.float32),
            pltpu.VMEM((width // LANES, rows, LANES), jnp.float32),
        ],
    )(
        rec, before, conv_weight, conv_bias.reshape(1, inner), table, gate_bias,
        decay_param.reshape(1, inner),
    )


def shards(
    nz, paired, tokens, norm_gain, lru_proj, gelu_proj, conv_weight, conv_bias, gate_weights,
    gate_bias, decay_param,
):
    seq_count, tok_rows, width = tokens.shape
    inner = lru_proj.shape[1]
    taps = conv_weight.shape[0]
    if paired:
        out = fused_branch(
            nz, tokens.reshape(tok_rows, width), norm_gain, lru_proj, gelu_proj, conv_weight,
            conv_bias, gate_weights, gate_bias, decay_param,
        )
        return out.reshape(seq_count, tok_rows, inner)
    flat = tokens.reshape(tok_rows, width).astype(jnp.float32)
    mean_square = jnp.mean(flat * flat, axis=-1, keepdims=True)
    normed = (flat * lax.rsqrt(mean_square + 1e-06) * norm_gain).astype(jnp.bfloat16)
    every = [
        lax.all_gather(w, ("fsdp", "seq"), axis=0, tiled=True) for w in (lru_proj, gelu_proj)
    ]
    rec = jnp.dot(normed, every[0], preferred_element_type=jnp.float32).astype(jnp.bfloat16)
    act = jnp.dot(normed, every[1], preferred_element_type=jnp.float32)
    table = lax.all_gather(gate_weights, "seq", axis=0, tiled=True)
    lead = 8
    before = lax.ppermute(
        rec[tok_rows - lead :, :], "seq", [(i, i + 1) for i in range(nz - 1)]
    )
    local, cumulative, ends = local_scan(
        rec, before, conv_weight, conv_bias, table, gate_bias, decay_param
    )
    every_end = lax.all_gather(ends, "seq")
    position = lax.axis_index("seq")
    start = jnp.zeros((inner,), jnp.float32)
    for k in range(nz - 1):
        start = jnp.where(k < position, every_end[k, 0] * start + every_end[k, 1], start)
    gelu = jax.nn.gelu(act, approximate=True)
    out = ((local + cumulative * start) * gelu).astype(jnp.bfloat16)
    return out.reshape(seq_count, tok_rows, inner)


def solution(mesh):
    placed = (
        P("fsdp", "seq", None), P(), P(("fsdp", "seq"), None), P(("fsdp", "seq"), None), P(), P(),
        P("seq", None), P(), P(),
    )
    nz = mesh.shape["seq"]
    paired = mesh.shape["fsdp"] == 8 and nz == len(LAGS) - 1
    return jax.shard_map(
        functools.partial(shards, nz, paired), mesh=mesh, in_specs=placed,
        out_specs=P("fsdp", "seq", None), check_vma=False,
    )
```

```python
import functools

import jax
import jax.numpy as jnp
from jax import lax
from jax.experimental import pallas as pl
from jax.experimental.pallas import tpu as pltpu
from jax.sharding import PartitionSpec as P

MESH = pl.DeviceIdType.MESH
LANES = 128
VMEM_BYTES = 58_000_000


def normalise(normed_ref, gain_ref, part, parts):
    rows = 32

    def body(i, _):
        at = pl.ds(pl.multiple_of(i * rows, rows), rows)
        values = normed_ref[at, :].astype(jnp.float32)
        mean_square = jnp.mean(values * values, axis=-1, keepdims=True)
        normed_ref[at, :] = (values * lax.rsqrt(mean_square + 1e-06) * gain_ref[...]).astype(jnp.bfloat16)
        return 0

    blocks = normed_ref.shape[0] // rows // parts
    lax.fori_loop(part * blocks, (part + 1) * blocks, body, 0)


LAGS = (6, 11, 14, 16, 17)
NORM_PARTS = 4
TALL = 512
EXTRA = 1
SLACK = 0


def hop_counts(nz, k, early, gates):
    last, reach = nz - 1, nz - 2
    twice = 2 if gates else 1
    end = k in (0, last)
    got = {0: 2, 1: 1}
    for distance in range(1, nz):
        sources = int(k >= distance) + int(k + distance < nz)
        got[distance - 1] = got.get(distance - 1, 0) + twice * sources
        if distance <= reach:
            for source in (k - distance, k + distance):
                if 0 <= source < nz and not (early and end and distance == reach):
                    got[distance + 1] = got.get(distance + 1, 0) + 1
    got[last] = got.get(last, 0) + 2 * last
    far = (2 if early else 1) if end else 0
    sent = 2 + 2 * last + 1 + far
    for source in range(nz):
        for target in (k - 1, k + 1):
            onward = (target - k) * (k - source) >= 0
            if not (0 <= target < nz and onward):
                continue
            sent += 1
            distance = abs(target - source)
            closed = early and target in (0, last) and distance == reach
            if distance <= reach and not closed:
                sent += 1
    passed = sum(
        1 for source in range(nz) for target in (k - 1, k + 1)
        if 0 <= target < nz and (target - k) * (k - source) >= 0
    )
    return got, far, sent, passed


def branch_kernel(
    nz,
    tokens_ref, gain_in, lru_ref, gelu_ref, gate_ref,
    weight_in, bias_in, gate_bias_in, decay_in,
    out_ref,
    gain_ref, weight_ref, bias_ref, gate_bias_ref, decay_ref,
    w_ref, normed_ref, rec_ref, table_ref, before_ref, padded_ref, a_ref, b_ref,
    end_ref, carry_ref, start_ref,
    own_sem, out_sem, send_sem, core_send, gate_send, gate_core_send, tail_send, carry_send,
    hop_recv, far_recv, core_recv, gate_core_recv, tail_recv, carry_recv,
):
    f = lax.axis_index("fsdp")
    z = lax.axis_index("seq")
    c, x, y = f % 2, (f // 2) % 2, f // 4
    fx, fy, fc = f + 2 - 4 * x, f + 4 - 8 * y, f + 1 - 2 * c
    fd = fx + 4 - 8 * y
    shard = lru_ref.shape[0]
    line = shard * nz
    half = shard // 2
    chunks, _, wide = w_ref.shape
    split = chunks // 2
    early_chunks = split + EXTRA
    gate_rows = gate_ref.shape[0]
    gate_steps = split // 2
    piece = gate_rows // 2 // gate_steps
    rows = normed_ref.shape[0]
    channels = table_ref.shape[1] // 2
    heads = rec_ref.shape[1] // channels
    pieces = channels // LANES
    taps = weight_ref.shape[0]
    lead = before_ref.shape[0]
    last = nz - 1
    reach = nz - 2
    at_end = (z == 0) | (z == last)

    def remote(src, send, recv, device):
        return pltpu.make_async_remote_copy(
            src_ref=src, dst_ref=src, send_sem=send, recv_sem=recv,
            device_id=device, device_id_type=MESH,
        )

    own = pl.ds(pl.multiple_of((f * nz + z) * shard, shard), shard)
    for t in range(chunks):
        src = lru_ref if t < split else gelu_ref
        cols = pl.ds((t % split) * wide, wide)
        pltpu.make_async_copy(src.at[:, cols], w_ref.at[t, own], own_sem.at[0]).start()
    own_gate = pl.ds(pl.multiple_of(z * gate_rows, gate_rows), gate_rows)
    gate_copy = pltpu.make_async_copy(gate_ref, table_ref.at[own_gate], own_sem.at[1])
    gate_copy.start()
    token_copy = pltpu.make_async_copy(tokens_ref, normed_ref, own_sem.at[2])
    token_copy.start()
    small = [
        pltpu.make_async_copy(source, target, own_sem.at[3 + i])
        for i, (source, target) in enumerate((
            (gain_in, gain_ref), (weight_in, weight_ref), (bias_in, bias_ref),
            (gate_bias_in, gate_bias_ref), (decay_in, decay_ref),
        ))
    ]
    for copy in small:
        copy.start()

    barrier = pltpu.get_barrier_semaphore()
    for device in ((fx, z), (fy, z), (fc, z)):
        pl.semaphore_signal(barrier, inc=1, device_id=device, device_id_type=MESH)

    @pl.when(z > 0)
    def _():
        pl.semaphore_signal(barrier, inc=1, device_id=(f, z - 1), device_id_type=MESH)

    @pl.when(z < last)
    def _():
        pl.semaphore_signal(barrier, inc=1, device_id=(f, z + 1), device_id_type=MESH)

    for k in range(nz):
        @pl.when(z == k)
        def _():
            pl.semaphore_wait(barrier, 3 + int(k > 0) + int(k < last))

    pltpu.make_async_copy(w_ref.at[:, own], w_ref.at[:, own], own_sem.at[0]).wait()
    gate_copy.wait()

    def unit(t, owner, k, first=0, size=shard):
        start = (owner * nz + k) * shard + first
        return w_ref.at[t, pl.ds(pl.multiple_of(start, half), size)]

    def whole_line(t, owner):
        return w_ref.at[t, pl.ds(pl.multiple_of(owner * line, line), line)]

    def gate_of(t, source):
        first = source * gate_rows + c * (gate_rows // 2) + t * piece
        return table_ref.at[pl.ds(pl.multiple_of(first, piece), piece)]

    core = core_send.at[0]

    def sender(t):
        return send_sem.at[jnp.where(t < early_chunks, 0, 1)]

    def along_z(t, k, target, distance):
        remote(unit(t, f, k), sender(t), hop_recv.at[t, distance - 1], (f, target)).start()

        @pl.when(t < gate_steps)
        def _():
            remote(gate_of(t, k), gate_send.at[0], hop_recv.at[t, distance - 1], (f, target)).start()

    def across(t, k, hop):
        remote(unit(t, f, k), sender(t), hop_recv.at[t, hop], (fx, z)).start()
        remote(unit(t, f, k), sender(t), hop_recv.at[t, hop], (fy, z)).start()

    def diagonal(t, k, target, distance):
        remote(unit(t, fd, k), sender(t), hop_recv.at[t, distance + 1], (f, target)).start()

    def wait_hop(t, hop):
        sizes = {}
        for k in range(nz):
            for early, gates in ((True, True), (True, False), (False, False)):
                count = hop_counts(nz, k, early, gates)[0].get(hop, 0)
                sizes.setdefault(count, {}).setdefault((early, gates), []).append(k)
        for count, places in sizes.items():
            if count == 0:
                continue
            chosen = False
            for (early, gates), ks in places.items():
                when = (t < gate_steps) if gates else ((t >= gate_steps) & (t < early_chunks)) if early else (t >= early_chunks)
                if len(ks) < nz:
                    there = z == ks[0]
                    for k in ks[1:]:
                        there = there | (z == k)
                    when = when & there
                chosen = when if chosen is False else chosen | when

            @pl.when(chosen)
            def _():
                block = w_ref.at[0, pl.ds(0, count * shard)]
                pltpu.make_async_copy(block, block, hop_recv.at[t, hop]).wait()

    def own_first(t):
        @pl.when(z > 0)
        def _():
            along_z(t, z, z - 1, 1)

        @pl.when(z < last)
        def _():
            along_z(t, z, z + 1, 1)

        across(t, z, 0)

    def z_hop(t, distance):
        @pl.when((z >= distance) & (z < last))
        def _():
            along_z(t, z - distance, z + 1, distance + 1)

        @pl.when((z + distance < nz) & (z > 0))
        def _():
            along_z(t, z + distance, z - 1, distance + 1)

    def sideways(t, distance):
        @pl.when(z >= distance)
        def _():
            across(t, z - distance, last)

        @pl.when(z + distance < nz)
        def _():
            across(t, z + distance, last)

    def d_hop(t, distance):
        onward = (t >= early_chunks) | (distance + 1 < reach)

        @pl.when((z >= distance) & (z < last) & (onward | (z + 1 < last)))
        def _():
            diagonal(t, z - distance, z + 1, distance + 1)

        @pl.when((z + distance < nz) & (z > 0) & (onward | (z - 1 > 0)))
        def _():
            diagonal(t, z + distance, z - 1, distance + 1)

    far = last - z
    middle = jnp.where(z == 0, reach, 1)

    def hop_done(t, hop):
        wait_hop(t, hop)
        if hop + 1 < last:
            z_hop(t, hop + 1)
        if hop == 0:
            remote(unit(t, fx, z, 0, half), sender(t), hop_recv.at[t, 1], (fy, z)).start()
            remote(unit(t, fy, z, half, half), sender(t), hop_recv.at[t, 1], (fx, z)).start()
        if hop == 1:
            @pl.when(z > 0)
            def _():
                diagonal(t, z, z - 1, 1)

            @pl.when(z < last)
            def _():
                diagonal(t, z, z + 1, 1)
        if 2 <= hop < last:
            d_hop(t, hop - 1)
        if hop + 1 <= last:
            sideways(t, hop + 1)
        if hop + 1 == last:
            remote(whole_line(t, f), core, core_recv.at[t], (fc, z)).start()

            @pl.when(t < gate_steps)
            def _():
                for k in range(nz):
                    @pl.when(z != k)
                    def _():
                        remote(gate_of(t, k), gate_core_send.at[0], gate_core_recv.at[0], (fc, z)).start()
        if hop == last:
            @pl.when(at_end & (t < early_chunks))
            def _():
                remote(unit(t, fx, far), sender(t), far_recv.at[t], (fy, z)).start()
                remote(unit(t, fy, middle), sender(t), far_recv.at[t], (fx, z)).start()

            @pl.when(at_end & (t >= early_chunks))
            def _():
                remote(unit(t, fx, far, 0, half), sender(t), far_recv.at[t], (fy, z)).start()
                remote(unit(t, fy, far, half, half), sender(t), far_recv.at[t], (fx, z)).start()

            remote(whole_line(t, fx), core, core_recv.at[t], (fc, z)).start()
            remote(whole_line(t, fy), core, core_recv.at[t], (fc, z)).start()

    def corner_done(t):
        @pl.when(at_end & (t < early_chunks))
        def _():
            block = w_ref.at[0, pl.ds(0, 2 * shard)]
            pltpu.make_async_copy(block, block, far_recv.at[t]).wait()

        @pl.when(at_end & (t >= early_chunks))
        def _():
            block = w_ref.at[0, pl.ds(0, shard)]
            pltpu.make_async_copy(block, block, far_recv.at[t]).wait()

        remote(whole_line(t, fd), core, core_recv.at[t], (fc, z)).start()

    def multiply(t):
        whole = w_ref.at[t, pl.ds(0, 4 * line)]
        pltpu.make_async_copy(whole, whole, core_recv.at[t]).wait()
        column = columns(t % split)
        tall = TALL

        def body(i, _):
            at = pl.ds(pl.multiple_of(i * tall, tall), tall)
            product = jnp.dot(normed_ref[at, :], w_ref[t], preferred_element_type=jnp.float32)

            @pl.when(t < split)
            def _():
                rec_ref[at, column] = product.astype(jnp.bfloat16)

            @pl.when(t >= split)
            def _():
                h = jnp.maximum(t - split, 0)
                for j in range(pieces):
                    lanes = pl.ds(pl.multiple_of(h * channels + j * LANES, LANES), LANES)
                    state = b_ref[h * pieces + j, at, :] + a_ref[h * pieces + j, at, :] * start_ref[h, :, j * LANES : (j + 1) * LANES]
                    act = jax.nn.gelu(product[:, j * LANES : (j + 1) * LANES], approximate=True)
                    out_ref[at, lanes] = (state * act).astype(out_ref.dtype)

            return 0

        lax.fori_loop(0, rows // tall, body, 0)

    def columns(h):
        return pl.ds(pl.multiple_of(h * channels, channels), channels)

    def tail_copy(h, source_rows, device):
        return pltpu.make_async_remote_copy(
            src_ref=rec_ref.at[pl.ds(source_rows, lead), columns(h)],
            dst_ref=before_ref.at[:, columns(h)],
            send_sem=tail_send.at[0], recv_sem=tail_recv.at[h],
            device_id=device, device_id_type=MESH,
        )

    def carry_copy(h, device):
        return pltpu.make_async_remote_copy(
            src_ref=carry_ref.at[h], dst_ref=start_ref.at[h],
            send_sem=carry_send.at[0], recv_sem=carry_recv.at[h],
            device_id=device, device_id_type=MESH,
        )

    def send_tail(h):
        @pl.when(z < last)
        def _():
            tail_copy(h, rows - lead, (f, z + 1)).start()

    def scan(h):
        @pl.when(z > 0)
        def _():
            tail_copy(h, rows - lead, (f, z)).wait_recv()

        cols = columns(h)
        padded_ref[pl.ds(0, lead), :] = before_ref[:, cols].astype(jnp.float32)
        padded_ref[pl.ds(lead, rows), :] = rec_ref[:, cols].astype(jnp.float32)
        conv_sum = jnp.zeros((rows, channels), jnp.float32) + bias_ref[:, cols]
        for tap in range(taps):
            conv_sum = conv_sum + weight_ref[tap : tap + 1, cols] * padded_ref[pl.ds(lead - tap, rows), :]
        conv_out = conv_sum.astype(jnp.bfloat16)
        gates = jnp.dot(conv_out, table_ref[cols, :], preferred_element_type=jnp.float32)
        input_gate = jax.nn.sigmoid(gates[:, :channels] + gate_bias_ref[0:1, cols])
        recur_gate = jax.nn.sigmoid(gates[:, channels:] + gate_bias_ref[1:2, cols])
        param = decay_ref[:, cols]
        softplus = jnp.maximum(param, 0.0) + jnp.log1p(jnp.exp(-jnp.abs(param)))
        log_decay = -8.0 * softplus * recur_gate
        decay = jnp.exp(log_decay)
        lost = -jnp.tanh(log_decay) * (decay * decay + 1.0)
        driven = jnp.sqrt(lost) * input_gate * conv_out.astype(jnp.float32)
        for j in range(pieces):
            a_ref[h * pieces + j] = decay[:, j * LANES : (j + 1) * LANES]
            b_ref[h * pieces + j] = driven[:, j * LANES : (j + 1) * LANES]

        lanes = 8
        length = rows // lanes

        def body(i, carry):
            at = pl.ds(i, lanes, stride=length)
            after = []
            for j in range(pieces):
                product, state = carry[j]
                decay_now = a_ref[h * pieces + j, at, :]
                product = product * decay_now
                state = decay_now * state + b_ref[h * pieces + j, at, :]
                a_ref[h * pieces + j, at, :] = product
                b_ref[h * pieces + j, at, :] = state
                after.append((product, state))
            return tuple(after)

        fresh = (jnp.ones((lanes, LANES), jnp.float32), jnp.zeros((lanes, LANES), jnp.float32))
        totals = lax.fori_loop(0, length, body, (fresh,) * pieces, unroll=8)
        for j in range(pieces):
            product, state = totals[j]
            start = jnp.zeros((1, LANES), jnp.float32)
            prefix = jnp.ones((1, LANES), jnp.float32)
            for i in range(lanes):
                at = pl.ds(i * length, length)
                within = a_ref[h * pieces + j, at, :]
                b_ref[h * pieces + j, at, :] = b_ref[h * pieces + j, at, :] + within * start
                a_ref[h * pieces + j, at, :] = within * prefix
                start = product[i : i + 1, :] * start + state[i : i + 1, :]
                prefix = prefix * product[i : i + 1, :]
            col = pl.ds(pl.multiple_of((h * pieces + j) * LANES, LANES), LANES)
            end_ref[0:1, col] = prefix
            end_ref[1:2, col] = start

    def make_carry(h):
        cols = columns(h)

        @pl.when(z > 0)
        def _():
            carry_copy(h, (f, z)).wait_recv()

        @pl.when(z < last)
        def _():
            carry_ref[h] = end_ref[0:1, cols] * start_ref[h] + end_ref[1:2, cols]

    def send_carry(h):
        @pl.when(z < last)
        def _():
            carry_copy(h, (f, z + 1)).start()

    @pl.when(z == 0)
    def _():
        before_ref[...] = jnp.zeros_like(before_ref)
        start_ref[...] = jnp.zeros_like(start_ref)

    hops = [(functools.partial(hop_done, hop=hop), LAGS[hop]) for hop in range(nz)]
    stages = hops[::-1] + [(corner_done, LAGS[nz]), (own_first, 0)]
    gates_at = LAGS[reach] + gate_steps
    finish = LAGS[nz] + 1
    tail_at = finish + 1
    scan_at = max(tail_at + 1 + SLACK, gates_at)
    steps = chunks + finish

    def on_head(s, first, stage):
        @pl.when((s >= first) & (s < first + heads))
        def _():
            stage(s - first)

    def step(s, _):
        on_head(s, scan_at + 2 + z, send_carry)
        on_head(s, tail_at, send_tail)

        for stage, lag in stages:
            @pl.when((s >= lag) & (s < chunks + lag))
            def _():
                stage(s - lag)

        @pl.when(s == gates_at)
        def _():
            others = table_ref.at[pl.ds(0, last * piece * gate_steps)]
            pltpu.make_async_copy(others, others, gate_core_recv.at[0]).wait()

        @pl.when(s == LAGS[0])
        def _():
            token_copy.wait()
            for copy in small:
                copy.wait()

        @pl.when((s >= LAGS[0]) & (s < LAGS[0] + NORM_PARTS))
        def _():
            normalise(normed_ref, gain_ref, s - LAGS[0], NORM_PARTS)

        @pl.when((s >= finish) & (s < chunks + finish))
        def _():
            multiply(s - finish)

        on_head(s, scan_at, scan)
        on_head(s, scan_at + 1 + z, make_carry)
        return 0

    lax.fori_loop(0, steps, step, 0)

    for k in range(nz):
        early, late = hop_counts(nz, k, True, False), hop_counts(nz, k, False, False)

        @pl.when(z == k)
        def _():
            for i, (depth, counts) in enumerate(((early_chunks, early), (chunks - early_chunks, late))):
                sent = w_ref.at[pl.ds(0, depth), pl.ds(0, counts[2] * shard)]
                pltpu.make_async_copy(sent, sent, send_sem.at[i]).wait()
            sent_gate = table_ref.at[pl.ds(0, early[3] * piece * gate_steps)]
            pltpu.make_async_copy(sent_gate, sent_gate, gate_send.at[0]).wait()

    whole = w_ref.at[:, pl.ds(0, 4 * line)]
    pltpu.make_async_copy(whole, whole, core).wait()
    others = table_ref.at[pl.ds(0, last * piece * gate_steps)]
    pltpu.make_async_copy(others, others, gate_core_send.at[0]).wait()

    @pl.when(z < last)
    def _():
        pltpu.make_async_copy(before_ref, before_ref, tail_send.at[0]).wait()
        pltpu.make_async_copy(carry_ref, carry_ref, carry_send.at[0]).wait()


def fused_branch(
    nz, tokens, norm_gain, lru_proj, gelu_proj, conv_weight, conv_bias, gate_weights, gate_bias,
    decay_param,
):
    rows, width = tokens.shape
    inner = lru_proj.shape[1]
    channels = gate_weights.shape[1] // 2
    chunks = 2 * inner // channels
    heads = inner // channels
    any_ = pl.BlockSpec(memory_space=pl.ANY)
    dma = pltpu.SemaphoreType.DMA
    f32, bf16 = jnp.float32, jnp.bfloat16
    lead = 8
    return pl.pallas_call(
        functools.partial(branch_kernel, nz),
        out_shape=pltpu.VMEM((rows, inner), bf16),
        in_specs=[any_] * 9,
        out_specs=pl.BlockSpec(memory_space=pltpu.VMEM),
        scratch_shapes=[
            pltpu.VMEM((1, width), f32), pltpu.VMEM(conv_weight.shape, f32), pltpu.VMEM((1, inner), f32),
            pltpu.VMEM(gate_bias.shape, f32), pltpu.VMEM((1, inner), f32),
            pltpu.VMEM((chunks, width, channels), bf16),
            pltpu.VMEM((rows, width), bf16),
            pltpu.VMEM((rows, inner), bf16),
            pltpu.VMEM((gate_weights.shape[0] * nz, 2 * channels), bf16),
            pltpu.VMEM((lead, inner), bf16),
            pltpu.VMEM((lead + rows, channels), f32),
            pltpu.VMEM((inner // LANES, rows, LANES), f32),
            pltpu.VMEM((inner // LANES, rows, LANES), f32),
            pltpu.VMEM((8, inner), f32), pltpu.VMEM((heads, 1, channels), f32), pltpu.VMEM((heads, 1, channels), f32),
            dma((8,)), dma((1,)), dma((2,)), dma((1,)), dma((1,)), dma((1,)), dma((1,)), dma((1,)),
            dma((chunks, nz)), dma((chunks,)), dma((chunks,)), dma((1,)),
            dma((heads,)), dma((heads,)),
        ],
        compiler_params=pltpu.CompilerParams(
            collective_id=0, has_side_effects=True, vmem_limit_bytes=VMEM_BYTES
        ),
    )(
        tokens, norm_gain.reshape(1, width), lru_proj, gelu_proj, gate_weights, conv_weight,
        conv_bias.reshape(1, inner), gate_bias, decay_param.reshape(1, inner),
    )


def scan_kernel(
    rec_ref, before_ref, weight_ref, bias_ref, table_ref, gate_bias_ref, decay_ref,
    state_ref, cumulative_ref, end_ref, padded_ref, a_ref, b_ref,
):
    rows, channels = rec_ref.shape
    taps = weight_ref.shape[0]
    lead = before_ref.shape[0]
    padded_ref[pl.ds(0, lead), :] = before_ref[...].astype(jnp.float32)
    padded_ref[pl.ds(lead, rows), :] = rec_ref[...].astype(jnp.float32)
    conv_sum = jnp.zeros((rows, channels), jnp.float32) + bias_ref[...]
    for tap in range(taps):
        conv_sum = conv_sum + weight_ref[tap : tap + 1, :] * padded_ref[pl.ds(lead - tap, rows), :]
    conv_out = conv_sum.astype(jnp.bfloat16)
    gates = jnp.dot(conv_out, table_ref[...], preferred_element_type=jnp.float32)
    input_gate = jax.nn.sigmoid(gates[:, :channels] + gate_bias_ref[0:1, :])
    recur_gate = jax.nn.sigmoid(gates[:, channels:] + gate_bias_ref[1:2, :])
    param = decay_ref[...]
    softplus = jnp.maximum(param, 0.0) + jnp.log1p(jnp.exp(-jnp.abs(param)))
    log_decay = -8.0 * softplus * recur_gate
    decay = jnp.exp(log_decay)
    lost = -jnp.tanh(log_decay) * (decay * decay + 1.0)
    driven = jnp.sqrt(lost) * input_gate * conv_out.astype(jnp.float32)
    parts = channels // LANES
    for j in range(parts):
        a_ref[j] = decay[:, j * LANES : (j + 1) * LANES]
        b_ref[j] = driven[:, j * LANES : (j + 1) * LANES]

    lanes = 8
    length = rows // lanes

    def body(i, carry):
        at = pl.ds(i, lanes, stride=length)
        after = []
        for j in range(parts):
            product, state = carry[j]
            decay_now = a_ref[j, at, :]
            product = product * decay_now
            state = decay_now * state + b_ref[j, at, :]
            a_ref[j, at, :] = product
            b_ref[j, at, :] = state
            after.append((product, state))
        return tuple(after)

    fresh = (jnp.ones((lanes, LANES), jnp.float32), jnp.zeros((lanes, LANES), jnp.float32))
    totals = lax.fori_loop(0, length, body, (fresh,) * parts, unroll=8)
    for j in range(parts):
        product, state = totals[j]
        cols = slice(j * LANES, (j + 1) * LANES)
        start = jnp.zeros((1, LANES), jnp.float32)
        prefix = jnp.ones((1, LANES), jnp.float32)
        for i in range(lanes):
            at = pl.ds(i * length, length)
            within = a_ref[j, at, :]
            state_ref[at, cols] = b_ref[j, at, :] + within * start
            cumulative_ref[at, cols] = within * prefix
            start = product[i : i + 1, :] * start + state[i : i + 1, :]
            prefix = prefix * product[i : i + 1, :]
        end_ref[0:1, cols] = prefix
        end_ref[1:2, cols] = start


def local_scan(rec, before, conv_weight, conv_bias, table, gate_bias, decay_param):
    rows, inner = rec.shape
    width = table.shape[1] // 2
    lead = before.shape[0]

    def columns(height):
        return pl.BlockSpec((height, width), lambda h: (0, h))

    return pl.pallas_call(
        scan_kernel,
        grid=(inner // width,),
        out_shape=(
            jax.ShapeDtypeStruct((rows, inner), jnp.float32),
            jax.ShapeDtypeStruct((rows, inner), jnp.float32),
            jax.ShapeDtypeStruct((2, inner), jnp.float32),
        ),
        in_specs=[
            columns(rows), columns(lead), columns(conv_weight.shape[0]), columns(1),
            pl.BlockSpec((width, 2 * width), lambda h: (h, 0)), columns(2), columns(1),
        ],
        out_specs=(columns(rows), columns(rows), columns(2)),
        scratch_shapes=[
            pltpu.VMEM((rows + lead, width), jnp.float32),
            pltpu.VMEM((width // LANES, rows, LANES), jnp.float32),
            pltpu.VMEM((width // LANES, rows, LANES), jnp.float32),
        ],
    )(
        rec, before, conv_weight, conv_bias.reshape(1, inner), table, gate_bias,
        decay_param.reshape(1, inner),
    )


def shards(
    nz, paired, tokens, norm_gain, lru_proj, gelu_proj, conv_weight, conv_bias, gate_weights,
    gate_bias, decay_param,
):
    seq_count, tok_rows, width = tokens.shape
    inner = lru_proj.shape[1]
    taps = conv_weight.shape[0]
    if paired:
        out = fused_branch(
            nz, tokens.reshape(tok_rows, width), norm_gain, lru_proj, gelu_proj, conv_weight,
            conv_bias, gate_weights, gate_bias, decay_param,
        )
        return out.reshape(seq_count, tok_rows, inner)
    flat = tokens.reshape(tok_rows, width).astype(jnp.float32)
    mean_square = jnp.mean(flat * flat, axis=-1, keepdims=True)
    normed = (flat * lax.rsqrt(mean_square + 1e-06) * norm_gain).astype(jnp.bfloat16)
    every = [
        lax.all_gather(w, ("fsdp", "seq"), axis=0, tiled=True) for w in (lru_proj, gelu_proj)
    ]
    rec = jnp.dot(normed, every[0], preferred_element_type=jnp.float32).astype(jnp.bfloat16)
    act = jnp.dot(normed, every[1], preferred_element_type=jnp.float32)
    table = lax.all_gather(gate_weights, "seq", axis=0, tiled=True)
    lead = 8
    before = lax.ppermute(
        rec[tok_rows - lead :, :], "seq", [(i, i + 1) for i in range(nz - 1)]
    )
    local, cumulative, ends = local_scan(
        rec, before, conv_weight, conv_bias, table, gate_bias, decay_param
    )
    every_end = lax.all_gather(ends, "seq")
    position = lax.axis_index("seq")
    start = jnp.zeros((inner,), jnp.float32)
    for k in range(nz - 1):
        start = jnp.where(k < position, every_end[k, 0] * start + every_end[k, 1], start)
    gelu = jax.nn.gelu(act, approximate=True)
    out = ((local + cumulative * start) * gelu).astype(jnp.bfloat16)
    return out.reshape(seq_count, tok_rows, inner)


def solution(mesh):
    placed = (
        P("fsdp", "seq", None), P(), P(("fsdp", "seq"), None), P(("fsdp", "seq"), None), P(), P(),
        P("seq", None), P(), P(),
    )
    nz = mesh.shape["seq"]
    paired = mesh.shape["fsdp"] == 8 and nz == len(LAGS) - 1
    return jax.shard_map(
        functools.partial(shards, nz, paired), mesh=mesh, in_specs=placed,
        out_specs=P("fsdp", "seq", None), check_vma=False,
    )
```

```python
import functools

import jax
import jax.numpy as jnp
from jax import lax
from jax.experimental import pallas as pl
from jax.experimental.pallas import tpu as pltpu
from jax.sharding import PartitionSpec as P

MESH = pl.DeviceIdType.MESH
LANES = 128
VMEM_BYTES = 58_000_000


def normalise(normed_ref, gain_ref, part, parts):
    rows = 32

    def body(i, _):
        at = pl.ds(pl.multiple_of(i * rows, rows), rows)
        values = normed_ref[at, :].astype(jnp.float32)
        mean_square = jnp.mean(values * values, axis=-1, keepdims=True)
        normed_ref[at, :] = (values * lax.rsqrt(mean_square + 1e-06) * gain_ref[...]).astype(jnp.bfloat16)
        return 0

    blocks = normed_ref.shape[0] // rows // parts
    lax.fori_loop(part * blocks, (part + 1) * blocks, body, 0)


LAGS = (6, 11, 14, 16, 17)
NORM_PARTS = 4
TALL = 512
EXTRA = 2
LONG = 2
SLACK = 0


def hop_counts(nz, k, early, gates):
    last, reach = nz - 1, nz - 2
    twice = 2 if gates else 1
    end = k in (0, last)
    got = {0: 2, 1: 1}
    for distance in range(1, nz):
        sources = int(k >= distance) + int(k + distance < nz)
        got[distance - 1] = got.get(distance - 1, 0) + twice * sources
        if distance <= reach:
            for source in (k - distance, k + distance):
                if 0 <= source < nz and not (early and end and distance == reach):
                    got[distance + 1] = got.get(distance + 1, 0) + 1
    got[last] = got.get(last, 0) + 2 * last
    far = (2 if early else 1) if end else 0
    sent = 2 + 2 * last + 1 + far
    for source in range(nz):
        for target in (k - 1, k + 1):
            onward = (target - k) * (k - source) >= 0
            if not (0 <= target < nz and onward):
                continue
            sent += 1
            distance = abs(target - source)
            closed = early and target in (0, last) and distance == reach
            if distance <= reach and not closed:
                sent += 1
    passed = sum(
        1 for source in range(nz) for target in (k - 1, k + 1)
        if 0 <= target < nz and (target - k) * (k - source) >= 0
    )
    return got, far, sent, passed


def branch_kernel(
    nz,
    tokens_ref, gain_in, lru_ref, gelu_ref, gate_ref,
    weight_in, bias_in, gate_bias_in, decay_in,
    out_ref,
    gain_ref, weight_ref, bias_ref, gate_bias_ref, decay_ref,
    w_ref, normed_ref, rec_ref, table_ref, before_ref, padded_ref, a_ref, b_ref,
    end_ref, carry_ref, start_ref,
    own_sem, out_sem, send_sem, core_send, gate_send, gate_core_send, tail_send, carry_send,
    hop_recv, far_recv, core_recv, gate_core_recv, tail_recv, carry_recv,
):
    f = lax.axis_index("fsdp")
    z = lax.axis_index("seq")
    c, x, y = f % 2, (f // 2) % 2, f // 4
    fx, fy, fc = f + 2 - 4 * x, f + 4 - 8 * y, f + 1 - 2 * c
    fd = fx + 4 - 8 * y
    shard = lru_ref.shape[0]
    line = shard * nz
    half = shard // 2
    chunks, _, wide = w_ref.shape
    split = chunks // 2
    early_chunks = split + EXTRA
    long_from = chunks - LONG
    gate_rows = gate_ref.shape[0]
    gate_steps = split // 2
    piece = gate_rows // 2 // gate_steps
    rows = normed_ref.shape[0]
    channels = table_ref.shape[1] // 2
    heads = rec_ref.shape[1] // channels
    pieces = channels // LANES
    taps = weight_ref.shape[0]
    lead = before_ref.shape[0]
    last = nz - 1
    reach = nz - 2
    at_end = (z == 0) | (z == last)

    def remote(src, send, recv, device):
        return pltpu.make_async_remote_copy(
            src_ref=src, dst_ref=src, send_sem=send, recv_sem=recv,
            device_id=device, device_id_type=MESH,
        )

    own = pl.ds(pl.multiple_of((f * nz + z) * shard, shard), shard)
    for t in range(chunks):
        src = lru_ref if t < split else gelu_ref
        cols = pl.ds((t % split) * wide, wide)
        pltpu.make_async_copy(src.at[:, cols], w_ref.at[t, own], own_sem.at[0]).start()
    own_gate = pl.ds(pl.multiple_of(z * gate_rows, gate_rows), gate_rows)
    gate_copy = pltpu.make_async_copy(gate_ref, table_ref.at[own_gate], own_sem.at[1])
    gate_copy.start()
    token_copy = pltpu.make_async_copy(tokens_ref, normed_ref, own_sem.at[2])
    token_copy.start()
    small = [
        pltpu.make_async_copy(source, target, own_sem.at[3 + i])
        for i, (source, target) in enumerate((
            (gain_in, gain_ref), (weight_in, weight_ref), (bias_in, bias_ref),
            (gate_bias_in, gate_bias_ref), (decay_in, decay_ref),
        ))
    ]
    for copy in small:
        copy.start()

    barrier = pltpu.get_barrier_semaphore()
    for device in ((fx, z), (fy, z), (fc, z)):
        pl.semaphore_signal(barrier, inc=1, device_id=device, device_id_type=MESH)

    @pl.when(z > 0)
    def _():
        pl.semaphore_signal(barrier, inc=1, device_id=(f, z - 1), device_id_type=MESH)

    @pl.when(z < last)
    def _():
        pl.semaphore_signal(barrier, inc=1, device_id=(f, z + 1), device_id_type=MESH)

    for k in range(nz):
        @pl.when(z == k)
        def _():
            pl.semaphore_wait(barrier, 3 + int(k > 0) + int(k < last))

    pltpu.make_async_copy(w_ref.at[:, own], w_ref.at[:, own], own_sem.at[0]).wait()
    gate_copy.wait()

    def unit(t, owner, k, first=0, size=shard):
        start = (owner * nz + k) * shard + first
        return w_ref.at[t, pl.ds(pl.multiple_of(start, half), size)]

    def whole_line(t, owner):
        return w_ref.at[t, pl.ds(pl.multiple_of(owner * line, line), line)]

    def gate_of(t, source):
        first = source * gate_rows + c * (gate_rows // 2) + t * piece
        return table_ref.at[pl.ds(pl.multiple_of(first, piece), piece)]

    core = core_send.at[0]

    def sender(t):
        return send_sem.at[jnp.where(t < early_chunks, 0, jnp.where(t < long_from, 1, 2))]

    def along_z(t, k, target, distance):
        remote(unit(t, f, k), sender(t), hop_recv.at[t, distance - 1], (f, target)).start()

        @pl.when(t < gate_steps)
        def _():
            remote(gate_of(t, k), gate_send.at[0], hop_recv.at[t, distance - 1], (f, target)).start()

    def across(t, k, hop):
        remote(unit(t, f, k), sender(t), hop_recv.at[t, hop], (fx, z)).start()
        remote(unit(t, f, k), sender(t), hop_recv.at[t, hop], (fy, z)).start()

    def diagonal(t, k, target, distance):
        if distance < reach:
            remote(unit(t, fd, k), sender(t), hop_recv.at[t, distance + 1], (f, target)).start()
            return
        apart = (t >= long_from) & (target > 0) & (target < last)

        @pl.when(apart)
        def _():
            remote(unit(t, fd, k), sender(t), far_recv.at[t], (f, target)).start()

        @pl.when(jnp.logical_not(apart))
        def _():
            remote(unit(t, fd, k), sender(t), hop_recv.at[t, distance + 1], (f, target)).start()

    def wait_hop(t, hop):
        spans = (
            (True, True, 0, t < gate_steps),
            (True, False, 0, (t >= gate_steps) & (t < early_chunks)),
            (False, False, 0, (t >= early_chunks) & (t < long_from)),
            (False, False, 1, t >= long_from),
        )
        sizes = {}
        for k in range(nz):
            for i, (early, gates, apart, _) in enumerate(spans):
                count = hop_counts(nz, k, early, gates)[0].get(hop, 0)
                if apart and hop == last and 0 < k < last:
                    count -= 1
                sizes.setdefault(count, {}).setdefault(i, []).append(k)
        for count, places in sizes.items():
            if count == 0:
                continue
            chosen = False
            for i, ks in places.items():
                when = spans[i][3]
                if len(ks) < nz:
                    there = z == ks[0]
                    for k in ks[1:]:
                        there = there | (z == k)
                    when = when & there
                chosen = when if chosen is False else chosen | when

            @pl.when(chosen)
            def _():
                block = w_ref.at[0, pl.ds(0, count * shard)]
                pltpu.make_async_copy(block, block, hop_recv.at[t, hop]).wait()

    def own_first(t):
        @pl.when(z > 0)
        def _():
            along_z(t, z, z - 1, 1)

        @pl.when(z < last)
        def _():
            along_z(t, z, z + 1, 1)

        across(t, z, 0)

    def z_hop(t, distance):
        @pl.when((z >= distance) & (z < last))
        def _():
            along_z(t, z - distance, z + 1, distance + 1)

        @pl.when((z + distance < nz) & (z > 0))
        def _():
            along_z(t, z + distance, z - 1, distance + 1)

    def sideways(t, distance):
        @pl.when(z >= distance)
        def _():
            across(t, z - distance, last)

        @pl.when(z + distance < nz)
        def _():
            across(t, z + distance, last)

    def d_hop(t, distance):
        onward = (t >= early_chunks) | (distance + 1 < reach)

        @pl.when((z >= distance) & (z < last) & (onward | (z + 1 < last)))
        def _():
            diagonal(t, z - distance, z + 1, distance + 1)

        @pl.when((z + distance < nz) & (z > 0) & (onward | (z - 1 > 0)))
        def _():
            diagonal(t, z + distance, z - 1, distance + 1)

    far = last - z
    middle = jnp.where(z == 0, reach, 1)

    def pass_far(t):
        for k, source, target in ((1, last, 0), (reach, 0, last)):
            @pl.when((t >= long_from) & (z == k))
            def _():
                block = unit(t, fd, source)
                pltpu.make_async_copy(block, block, far_recv.at[t]).wait()
                remote(block, sender(t), far_recv.at[t], (f, target)).start()

    def hop_done(t, hop):
        wait_hop(t, hop)
        if hop + 1 < last:
            z_hop(t, hop + 1)
        if hop == 0:
            remote(unit(t, fx, z, 0, half), sender(t), hop_recv.at[t, 1], (fy, z)).start()
            remote(unit(t, fy, z, half, half), sender(t), hop_recv.at[t, 1], (fx, z)).start()
        if hop == 1:
            @pl.when(z > 0)
            def _():
                diagonal(t, z, z - 1, 1)

            @pl.when(z < last)
            def _():
                diagonal(t, z, z + 1, 1)
        if 2 <= hop < last:
            d_hop(t, hop - 1)
        if hop + 1 <= last:
            sideways(t, hop + 1)
        if hop + 1 == last:
            remote(whole_line(t, f), core, core_recv.at[t], (fc, z)).start()

            @pl.when(t < gate_steps)
            def _():
                for k in range(nz):
                    @pl.when(z != k)
                    def _():
                        remote(gate_of(t, k), gate_core_send.at[0], gate_core_recv.at[0], (fc, z)).start()
        if hop == last:
            @pl.when(at_end & (t < early_chunks))
            def _():
                remote(unit(t, fx, far), sender(t), far_recv.at[t], (fy, z)).start()
                remote(unit(t, fy, middle), sender(t), far_recv.at[t], (fx, z)).start()

            @pl.when(at_end & (t >= early_chunks) & (t < long_from))
            def _():
                remote(unit(t, fx, far, 0, half), sender(t), far_recv.at[t], (fy, z)).start()
                remote(unit(t, fy, far, half, half), sender(t), far_recv.at[t], (fx, z)).start()

            remote(whole_line(t, fx), core, core_recv.at[t], (fc, z)).start()
            remote(whole_line(t, fy), core, core_recv.at[t], (fc, z)).start()

    def corner_done(t):
        @pl.when(at_end & (t < early_chunks))
        def _():
            block = w_ref.at[0, pl.ds(0, 2 * shard)]
            pltpu.make_async_copy(block, block, far_recv.at[t]).wait()

        @pl.when(at_end & (t >= early_chunks))
        def _():
            block = w_ref.at[0, pl.ds(0, shard)]
            pltpu.make_async_copy(block, block, far_recv.at[t]).wait()

        remote(whole_line(t, fd), core, core_recv.at[t], (fc, z)).start()

    def multiply(t):
        whole = w_ref.at[t, pl.ds(0, 4 * line)]
        pltpu.make_async_copy(whole, whole, core_recv.at[t]).wait()
        column = columns(t % split)
        tall = TALL

        def body(i, _):
            at = pl.ds(pl.multiple_of(i * tall, tall), tall)
            product = jnp.dot(normed_ref[at, :], w_ref[t], preferred_element_type=jnp.float32)

            @pl.when(t < split)
            def _():
                rec_ref[at, column] = product.astype(jnp.bfloat16)

            @pl.when(t >= split)
            def _():
                h = jnp.maximum(t - split, 0)
                for j in range(pieces):
                    lanes = pl.ds(pl.multiple_of(h * channels + j * LANES, LANES), LANES)
                    state = b_ref[h * pieces + j, at, :] + a_ref[h * pieces + j, at, :] * start_ref[h, :, j * LANES : (j + 1) * LANES]
                    act = jax.nn.gelu(product[:, j * LANES : (j + 1) * LANES], approximate=True)
                    out_ref[at, lanes] = (state * act).astype(out_ref.dtype)

            return 0

        lax.fori_loop(0, rows // tall, body, 0)

    def columns(h):
        return pl.ds(pl.multiple_of(h * channels, channels), channels)

    def tail_copy(h, source_rows, device):
        return pltpu.make_async_remote_copy(
            src_ref=rec_ref.at[pl.ds(source_rows, lead), columns(h)],
            dst_ref=before_ref.at[:, columns(h)],
            send_sem=tail_send.at[0], recv_sem=tail_recv.at[h],
            device_id=device, device_id_type=MESH,
        )

    def carry_copy(h, device):
        return pltpu.make_async_remote_copy(
            src_ref=carry_ref.at[h], dst_ref=start_ref.at[h],
            send_sem=carry_send.at[0], recv_sem=carry_recv.at[h],
            device_id=device, device_id_type=MESH,
        )

    def send_tail(h):
        @pl.when(z < last)
        def _():
            tail_copy(h, rows - lead, (f, z + 1)).start()

    def scan(h):
        @pl.when(z > 0)
        def _():
            tail_copy(h, rows - lead, (f, z)).wait_recv()

        cols = columns(h)
        padded_ref[pl.ds(0, lead), :] = before_ref[:, cols].astype(jnp.float32)
        padded_ref[pl.ds(lead, rows), :] = rec_ref[:, cols].astype(jnp.float32)
        conv_sum = jnp.zeros((rows, channels), jnp.float32) + bias_ref[:, cols]
        for tap in range(taps):
            conv_sum = conv_sum + weight_ref[tap : tap + 1, cols] * padded_ref[pl.ds(lead - tap, rows), :]
        conv_out = conv_sum.astype(jnp.bfloat16)
        gates = jnp.dot(conv_out, table_ref[cols, :], preferred_element_type=jnp.float32)
        input_gate = jax.nn.sigmoid(gates[:, :channels] + gate_bias_ref[0:1, cols])
        recur_gate = jax.nn.sigmoid(gates[:, channels:] + gate_bias_ref[1:2, cols])
        param = decay_ref[:, cols]
        softplus = jnp.maximum(param, 0.0) + jnp.log1p(jnp.exp(-jnp.abs(param)))
        log_decay = -8.0 * softplus * recur_gate
        decay = jnp.exp(log_decay)
        lost = -jnp.tanh(log_decay) * (decay * decay + 1.0)
        driven = jnp.sqrt(lost) * input_gate * conv_out.astype(jnp.float32)
        for j in range(pieces):
            a_ref[h * pieces + j] = decay[:, j * LANES : (j + 1) * LANES]
            b_ref[h * pieces + j] = driven[:, j * LANES : (j + 1) * LANES]

        lanes = 8
        length = rows // lanes

        def body(i, carry):
            at = pl.ds(i, lanes, stride=length)
            after = []
            for j in range(pieces):
                product, state = carry[j]
                decay_now = a_ref[h * pieces + j, at, :]
                product = product * decay_now
                state = decay_now * state + b_ref[h * pieces + j, at, :]
                a_ref[h * pieces + j, at, :] = product
                b_ref[h * pieces + j, at, :] = state
                after.append((product, state))
            return tuple(after)

        fresh = (jnp.ones((lanes, LANES), jnp.float32), jnp.zeros((lanes, LANES), jnp.float32))
        totals = lax.fori_loop(0, length, body, (fresh,) * pieces, unroll=8)
        for j in range(pieces):
            product, state = totals[j]
            start = jnp.zeros((1, LANES), jnp.float32)
            prefix = jnp.ones((1, LANES), jnp.float32)
            for i in range(lanes):
                at = pl.ds(i * length, length)
                within = a_ref[h * pieces + j, at, :]
                b_ref[h * pieces + j, at, :] = b_ref[h * pieces + j, at, :] + within * start
                a_ref[h * pieces + j, at, :] = within * prefix
                start = product[i : i + 1, :] * start + state[i : i + 1, :]
                prefix = prefix * product[i : i + 1, :]
            col = pl.ds(pl.multiple_of((h * pieces + j) * LANES, LANES), LANES)
            end_ref[0:1, col] = prefix
            end_ref[1:2, col] = start

    def make_carry(h):
        cols = columns(h)

        @pl.when(z > 0)
        def _():
            carry_copy(h, (f, z)).wait_recv()

        @pl.when(z < last)
        def _():
            carry_ref[h] = end_ref[0:1, cols] * start_ref[h] + end_ref[1:2, cols]

    def send_carry(h):
        @pl.when(z < last)
        def _():
            carry_copy(h, (f, z + 1)).start()

    @pl.when(z == 0)
    def _():
        before_ref[...] = jnp.zeros_like(before_ref)
        start_ref[...] = jnp.zeros_like(start_ref)

    hops = [(functools.partial(hop_done, hop=hop), LAGS[hop]) for hop in range(nz)]
    stages = [(pass_far, LAGS[reach] + 1)] + hops[::-1] + [(corner_done, LAGS[nz]), (own_first, 0)]
    gates_at = LAGS[reach] + gate_steps
    finish = LAGS[nz] + 1
    tail_at = finish + 1
    scan_at = max(tail_at + 1 + SLACK, gates_at)
    steps = chunks + finish

    def on_head(s, first, stage):
        @pl.when((s >= first) & (s < first + heads))
        def _():
            stage(s - first)

    def step(s, _):
        on_head(s, scan_at + 2 + z, send_carry)
        on_head(s, tail_at, send_tail)

        for stage, lag in stages:
            @pl.when((s >= lag) & (s < chunks + lag))
            def _():
                stage(s - lag)

        @pl.when(s == gates_at)
        def _():
            others = table_ref.at[pl.ds(0, last * piece * gate_steps)]
            pltpu.make_async_copy(others, others, gate_core_recv.at[0]).wait()

        @pl.when(s == LAGS[0])
        def _():
            token_copy.wait()
            for copy in small:
                copy.wait()

        @pl.when((s >= LAGS[0]) & (s < LAGS[0] + NORM_PARTS))
        def _():
            normalise(normed_ref, gain_ref, s - LAGS[0], NORM_PARTS)

        @pl.when((s >= finish) & (s < chunks + finish))
        def _():
            multiply(s - finish)

        on_head(s, scan_at, scan)
        on_head(s, scan_at + 1 + z, make_carry)
        return 0

    lax.fori_loop(0, steps, step, 0)

    for k in range(nz):
        early, late = hop_counts(nz, k, True, False), hop_counts(nz, k, False, False)

        @pl.when(z == k)
        def _():
            through = late[2] - 1 if k in (0, last) else late[2] + int(k == 1) + int(k == reach)
            groups = ((early_chunks, early[2]), (long_from - early_chunks, late[2]), (LONG, through))
            for i, (depth, count) in enumerate(groups):
                sent = w_ref.at[pl.ds(0, depth), pl.ds(0, count * shard)]
                pltpu.make_async_copy(sent, sent, send_sem.at[i]).wait()
            sent_gate = table_ref.at[pl.ds(0, early[3] * piece * gate_steps)]
            pltpu.make_async_copy(sent_gate, sent_gate, gate_send.at[0]).wait()

    whole = w_ref.at[:, pl.ds(0, 4 * line)]
    pltpu.make_async_copy(whole, whole, core).wait()
    others = table_ref.at[pl.ds(0, last * piece * gate_steps)]
    pltpu.make_async_copy(others, others, gate_core_send.at[0]).wait()

    @pl.when(z < last)
    def _():
        pltpu.make_async_copy(before_ref, before_ref, tail_send.at[0]).wait()
        pltpu.make_async_copy(carry_ref, carry_ref, carry_send.at[0]).wait()


def fused_branch(
    nz, tokens, norm_gain, lru_proj, gelu_proj, conv_weight, conv_bias, gate_weights, gate_bias,
    decay_param,
):
    rows, width = tokens.shape
    inner = lru_proj.shape[1]
    channels = gate_weights.shape[1] // 2
    chunks = 2 * inner // channels
    heads = inner // channels
    any_ = pl.BlockSpec(memory_space=pl.ANY)
    dma = pltpu.SemaphoreType.DMA
    f32, bf16 = jnp.float32, jnp.bfloat16
    lead = 8
    return pl.pallas_call(
        functools.partial(branch_kernel, nz),
        out_shape=pltpu.VMEM((rows, inner), bf16),
        in_specs=[any_] * 9,
        out_specs=pl.BlockSpec(memory_space=pltpu.VMEM),
        scratch_shapes=[
            pltpu.VMEM((1, width), f32), pltpu.VMEM(conv_weight.shape, f32), pltpu.VMEM((1, inner), f32),
            pltpu.VMEM(gate_bias.shape, f32), pltpu.VMEM((1, inner), f32),
            pltpu.VMEM((chunks, width, channels), bf16),
            pltpu.VMEM((rows, width), bf16),
            pltpu.VMEM((rows, inner), bf16),
            pltpu.VMEM((gate_weights.shape[0] * nz, 2 * channels), bf16),
            pltpu.VMEM((lead, inner), bf16),
            pltpu.VMEM((lead + rows, channels), f32),
            pltpu.VMEM((inner // LANES, rows, LANES), f32),
            pltpu.VMEM((inner // LANES, rows, LANES), f32),
            pltpu.VMEM((8, inner), f32), pltpu.VMEM((heads, 1, channels), f32), pltpu.VMEM((heads, 1, channels), f32),
            dma((8,)), dma((1,)), dma((3,)), dma((1,)), dma((1,)), dma((1,)), dma((1,)), dma((1,)),
            dma((chunks, nz)), dma((chunks,)), dma((chunks,)), dma((1,)),
            dma((heads,)), dma((heads,)),
        ],
        compiler_params=pltpu.CompilerParams(
            collective_id=0, has_side_effects=True, vmem_limit_bytes=VMEM_BYTES
        ),
    )(
        tokens, norm_gain.reshape(1, width), lru_proj, gelu_proj, gate_weights, conv_weight,
        conv_bias.reshape(1, inner), gate_bias, decay_param.reshape(1, inner),
    )


def scan_kernel(
    rec_ref, before_ref, weight_ref, bias_ref, table_ref, gate_bias_ref, decay_ref,
    state_ref, cumulative_ref, end_ref, padded_ref, a_ref, b_ref,
):
    rows, channels = rec_ref.shape
    taps = weight_ref.shape[0]
    lead = before_ref.shape[0]
    padded_ref[pl.ds(0, lead), :] = before_ref[...].astype(jnp.float32)
    padded_ref[pl.ds(lead, rows), :] = rec_ref[...].astype(jnp.float32)
    conv_sum = jnp.zeros((rows, channels), jnp.float32) + bias_ref[...]
    for tap in range(taps):
        conv_sum = conv_sum + weight_ref[tap : tap + 1, :] * padded_ref[pl.ds(lead - tap, rows), :]
    conv_out = conv_sum.astype(jnp.bfloat16)
    gates = jnp.dot(conv_out, table_ref[...], preferred_element_type=jnp.float32)
    input_gate = jax.nn.sigmoid(gates[:, :channels] + gate_bias_ref[0:1, :])
    recur_gate = jax.nn.sigmoid(gates[:, channels:] + gate_bias_ref[1:2, :])
    param = decay_ref[...]
    softplus = jnp.maximum(param, 0.0) + jnp.log1p(jnp.exp(-jnp.abs(param)))
    log_decay = -8.0 * softplus * recur_gate
    decay = jnp.exp(log_decay)
    lost = -jnp.tanh(log_decay) * (decay * decay + 1.0)
    driven = jnp.sqrt(lost) * input_gate * conv_out.astype(jnp.float32)
    parts = channels // LANES
    for j in range(parts):
        a_ref[j] = decay[:, j * LANES : (j + 1) * LANES]
        b_ref[j] = driven[:, j * LANES : (j + 1) * LANES]

    lanes = 8
    length = rows // lanes

    def body(i, carry):
        at = pl.ds(i, lanes, stride=length)
        after = []
        for j in range(parts):
            product, state = carry[j]
            decay_now = a_ref[j, at, :]
            product = product * decay_now
            state = decay_now * state + b_ref[j, at, :]
            a_ref[j, at, :] = product
            b_ref[j, at, :] = state
            after.append((product, state))
        return tuple(after)

    fresh = (jnp.ones((lanes, LANES), jnp.float32), jnp.zeros((lanes, LANES), jnp.float32))
    totals = lax.fori_loop(0, length, body, (fresh,) * parts, unroll=8)
    for j in range(parts):
        product, state = totals[j]
        cols = slice(j * LANES, (j + 1) * LANES)
        start = jnp.zeros((1, LANES), jnp.float32)
        prefix = jnp.ones((1, LANES), jnp.float32)
        for i in range(lanes):
            at = pl.ds(i * length, length)
            within = a_ref[j, at, :]
            state_ref[at, cols] = b_ref[j, at, :] + within * start
            cumulative_ref[at, cols] = within * prefix
            start = product[i : i + 1, :] * start + state[i : i + 1, :]
            prefix = prefix * product[i : i + 1, :]
        end_ref[0:1, cols] = prefix
        end_ref[1:2, cols] = start


def local_scan(rec, before, conv_weight, conv_bias, table, gate_bias, decay_param):
    rows, inner = rec.shape
    width = table.shape[1] // 2
    lead = before.shape[0]

    def columns(height):
        return pl.BlockSpec((height, width), lambda h: (0, h))

    return pl.pallas_call(
        scan_kernel,
        grid=(inner // width,),
        out_shape=(
            jax.ShapeDtypeStruct((rows, inner), jnp.float32),
            jax.ShapeDtypeStruct((rows, inner), jnp.float32),
            jax.ShapeDtypeStruct((2, inner), jnp.float32),
        ),
        in_specs=[
            columns(rows), columns(lead), columns(conv_weight.shape[0]), columns(1),
            pl.BlockSpec((width, 2 * width), lambda h: (h, 0)), columns(2), columns(1),
        ],
        out_specs=(columns(rows), columns(rows), columns(2)),
        scratch_shapes=[
            pltpu.VMEM((rows + lead, width), jnp.float32),
            pltpu.VMEM((width // LANES, rows, LANES), jnp.float32),
            pltpu.VMEM((width // LANES, rows, LANES), jnp.float32),
        ],
    )(
        rec, before, conv_weight, conv_bias.reshape(1, inner), table, gate_bias,
        decay_param.reshape(1, inner),
    )


def shards(
    nz, paired, tokens, norm_gain, lru_proj, gelu_proj, conv_weight, conv_bias, gate_weights,
    gate_bias, decay_param,
):
    seq_count, tok_rows, width = tokens.shape
    inner = lru_proj.shape[1]
    taps = conv_weight.shape[0]
    if paired:
        out = fused_branch(
            nz, tokens.reshape(tok_rows, width), norm_gain, lru_proj, gelu_proj, conv_weight,
            conv_bias, gate_weights, gate_bias, decay_param,
        )
        return out.reshape(seq_count, tok_rows, inner)
    flat = tokens.reshape(tok_rows, width).astype(jnp.float32)
    mean_square = jnp.mean(flat * flat, axis=-1, keepdims=True)
    normed = (flat * lax.rsqrt(mean_square + 1e-06) * norm_gain).astype(jnp.bfloat16)
    every = [
        lax.all_gather(w, ("fsdp", "seq"), axis=0, tiled=True) for w in (lru_proj, gelu_proj)
    ]
    rec = jnp.dot(normed, every[0], preferred_element_type=jnp.float32).astype(jnp.bfloat16)
    act = jnp.dot(normed, every[1], preferred_element_type=jnp.float32)
    table = lax.all_gather(gate_weights, "seq", axis=0, tiled=True)
    lead = 8
    before = lax.ppermute(
        rec[tok_rows - lead :, :], "seq", [(i, i + 1) for i in range(nz - 1)]
    )
    local, cumulative, ends = local_scan(
        rec, before, conv_weight, conv_bias, table, gate_bias, decay_param
    )
    every_end = lax.all_gather(ends, "seq")
    position = lax.axis_index("seq")
    start = jnp.zeros((inner,), jnp.float32)
    for k in range(nz - 1):
        start = jnp.where(k < position, every_end[k, 0] * start + every_end[k, 1], start)
    gelu = jax.nn.gelu(act, approximate=True)
    out = ((local + cumulative * start) * gelu).astype(jnp.bfloat16)
    return out.reshape(seq_count, tok_rows, inner)


def solution(mesh):
    placed = (
        P("fsdp", "seq", None), P(), P(("fsdp", "seq"), None), P(("fsdp", "seq"), None), P(), P(),
        P("seq", None), P(), P(),
    )
    nz = mesh.shape["seq"]
    paired = mesh.shape["fsdp"] == 8 and nz == len(LAGS) - 1
    return jax.shard_map(
        functools.partial(shards, nz, paired), mesh=mesh, in_specs=placed,
        out_specs=P("fsdp", "seq", None), check_vma=False,
    )
```
